32 devices in a mesh: batch: 2 (over x), row: 4 (over z), col: 4 (over y, core).
Axes of the slice: x: 2, y: 2, z: 4, core: 2. Of those that a mesh axis runs over, the one named last changes fastest.
Arguments:
- left_op: bfloat16 [24576, 12288], P(('batch', 'row'), 'col'), parts along dimension 0
- left_start: float32 [24576, 128], P(('batch', 'row', 'col')), parts along dimension 0
- right_op: bfloat16 [24576, 12288], P(('batch', 'row'), 'col'), parts along dimension 0
- right_start: float32 [24576, 128], P(('batch', 'row', 'col')), parts along dimension 0
Outputs:
- output 1: float32 [24576, 128], P(('batch', 'row', 'col')), parts along dimension 0
- output 2: float32 [256, 128], P('batch'), parts along dimension 0
- output 3: float32 [24576, 128], P(('batch', 'row', 'col')), parts along dimension 0
- output 4: float32 [256, 128], P('batch'), parts along dimension 0
There are 2 independent parts. The reference program is written for one: setup_inputs(seed, part) draws one part's arguments, and reference() takes and returns one part's arrays. A program takes and returns all parts, laid end to end along the dimension named above; each array names one.
All inputs are finite; a program needn't handle non-finite values.
Results may differ from the reference program's by a relative error of at most 0.001.
Values are sent between devices in bfloat16 or wider.
A program may use at most 1 GiB of HBM per device.

```python
import jax
import jax.numpy as jnp
from jax import lax

N = 12288
N2 = 12288
S = 128
SWEEPS = 4


def build_operator(key, size):
    key_vec, key_val, key_noise = jax.random.split(key, 3)
    eig_basis = jax.random.normal(key_vec, (size, S), jnp.float32) * (size ** -0.5)
    levels = 1.5 * 4.0 ** jax.random.uniform(key_val, (S,), jnp.float32)
    noise_mat = jax.random.normal(key_noise, (size, size), jnp.float32) * (0.1 * size ** -0.5)
    full_mat = jnp.dot(eig_basis * levels, eig_basis.T) + noise_mat
    symmetric = 0.5 * (full_mat + full_mat.T) + 0.5 * jnp.eye(size, dtype=jnp.float32)
    return symmetric.astype(jnp.bfloat16)


def setup_inputs(seed: int = 0, part: int = 0) -> dict:
    base_key = jax.random.fold_in(jax.random.key(seed), part)
    key_left_op, key_left_start, key_right_op, key_right_start = jax.random.split(base_key, 4)
    return {
        "left_op": build_operator(key_left_op, N),
        "left_start": jax.random.normal(key_left_start, (N, S), jnp.float32),
        "right_op": build_operator(key_right_op, N2),
        "right_start": jax.random.normal(key_right_start, (N2, S), jnp.float32),
    }


def cholqr_step(y_mat, gram_mat):
    chol_low = jnp.linalg.cholesky(gram_mat)
    return lax.linalg.triangular_solve(chol_low, y_mat, left_side=False, lower=True, transpose_a=True)


def orthonormalize(y_mat):
    row_count = y_mat.shape[0]
    y_half = y_mat.astype(jnp.bfloat16)
    gram_one = jnp.dot(y_half.T, y_half, preferred_element_type=jnp.float32) / row_count
    y_one = cholqr_step(y_mat, gram_one)
    gram_two = jnp.dot(y_one.T, y_one, precision=lax.Precision.HIGHEST) / row_count
    return cholqr_step(y_one, gram_two)


def iterate(operator, start_block):
    def one_sweep(x_cur, unused):
        y_mat = jnp.dot(operator, x_cur.astype(jnp.bfloat16), preferred_element_type=jnp.float32)
        return orthonormalize(y_mat), None

    x_final, scan_rest = lax.scan(one_sweep, start_block, None, length=SWEEPS)
    z_mat = jnp.dot(operator, x_final.astype(jnp.bfloat16), preferred_element_type=jnp.float32)
    rayleigh = jnp.dot(x_final.T, z_mat, precision=lax.Precision.HIGHEST) / x_final.shape[0]
    return x_final, rayleigh


def reference(left_op, left_start, right_op, right_start):
    left_basis, left_rayleigh = iterate(left_op, left_start)
    right_basis, right_rayleigh = iterate(right_op, right_start)
    return (left_basis, left_rayleigh, right_basis, right_rayleigh)
```

```python
import functools

import jax
import jax.numpy as jnp
from jax import lax
from jax.experimental import pallas as pl
from jax.experimental.pallas import tpu as pltpu
from jax.sharding import PartitionSpec as P

SWEEPS = 4
CHUNKS = 2
MESH = pl.DeviceIdType.MESH
HIGHEST = lax.Precision.HIGHEST
OPS = (0, 1)
F32 = jnp.float32
BF16 = jnp.bfloat16


def dot(lhs, rhs, lhs_dim, rhs_dim, precision=None):
    dims = (((lhs_dim,), (rhs_dim,)), ((), ()))
    return lax.dot_general(lhs, rhs, dims, precision=precision, preferred_element_type=F32)


def split3(v):
    one = v.astype(BF16).astype(F32)
    rest = v - one
    two = rest.astype(BF16).astype(F32)
    return one, two, rest - two


def kernel(rows, col, left_op, left_start, right_op, right_start, left_basis, left_ray, right_basis, right_ray,
           a_v, xg, xz, xf, part, rsa, sb, rsb, yv, gp, g1, s1, g2, slots, gs, gw, mv,
           load_sem, rsa_ss, rsa_rs, rsb_ss, rsb_rs, g1_ss, g1_rs, g2_ss, g2_rs, sl_ss, sl_rs, g4_ss, g4_rs,
           zr_ss, zl_ss, z_rs, p_ss, p_rs):
    b, z, c = lax.axis_index("batch"), lax.axis_index("row"), lax.axis_index("col")
    y, k = c // 2, c % 2
    blk = a_v.shape[1]
    sub = blk // col
    piece = sub // CHUNKS
    total = blk * rows
    half, quarter = 64, 32

    def dev(zz, yy, kk):
        return (b, zz, 2 * yy + kk)

    def rcopy(src, dst, ss, rs, to):
        return pltpu.make_async_remote_copy(src_ref=src, dst_ref=dst, send_sem=ss, recv_sem=rs, device_id=to, device_id_type=MESH)

    partner, across = dev(z, y, 1 - k), dev(z, 1 - y, k)

    def load(op, j):
        src = (left_op, right_op)[op]
        rng = pl.ds(j * sub, sub)
        return pltpu.make_async_copy(src.at[rng], a_v.at[op, rng], load_sem.at[op, j])

    for op in OPS:
        for j in range(col):
            load(op, j).start()

    barrier = pltpu.get_barrier_semaphore()
    me = z * col + c
    count = rows * col
    for d in range(1, count):
        peer = lax.rem(me + d, count)
        pl.semaphore_signal(barrier, inc=1, device_id=(b, peer // col, lax.rem(peer, col)), device_id_type=MESH)
    pl.semaphore_wait(barrier, count - 1)

    def z_copy(op, slot, h, step):
        rng = pl.ds(h * piece, piece)
        to, ss = (dev(z + 1, y, k), zr_ss) if step > 0 else (dev(z - 1, y, k), zl_ss)
        return rcopy(xz.at[op, slot, rng], xz.at[op, slot, rng], ss.at[op, slot, h], z_rs.at[op, slot, h], to)

    def p_copy(op, slot, h):
        src = xz.at[op, slot, pl.ds(h * piece, piece)]
        dst = xg.at[op, pl.ds(c * sub + h * piece, piece)]
        return rcopy(src, dst, p_ss.at[op, slot, h], p_rs.at[op, c, h], dev(z, slot // 2, lax.rem(slot, 2)))

    def p_local(op, slot, h):
        src = xz.at[op, slot, pl.ds(h * piece, piece)]
        dst = xg.at[op, pl.ds(c * sub + h * piece, piece)]
        return pltpu.make_async_copy(src, dst, p_rs.at[op, c, h])

    def p_start(op, slot, h):
        @pl.when(slot == c)
        def _():
            p_local(op, slot, h).start()

        @pl.when(slot != c)
        def _():
            p_copy(op, slot, h).start()

    def spread_begin(op):
        for h in range(CHUNKS):
            @pl.when(z < rows - 1)
            def _():
                z_copy(op, z, h, 1).start()

            @pl.when(z > 0)
            def _():
                z_copy(op, z, h, -1).start()
        for h in range(CHUNKS):
            p_start(op, z, h)

    def spread_step(op, t):
        for h in range(CHUNKS):
            @pl.when(z - t >= 0)
            def _():
                slot = z - t
                z_copy(op, slot, h, 1).wait_recv()

                @pl.when(z < rows - 1)
                def _():
                    z_copy(op, slot, h, 1).start()

                p_start(op, slot, h)

            @pl.when(z + t < rows)
            def _():
                slot = z + t
                z_copy(op, slot, h, -1).wait_recv()

                @pl.when(z > 0)
                def _():
                    z_copy(op, slot, h, -1).start()

                p_start(op, slot, h)

    def spread_end(op):
        for src in range(col):
            for h in range(CHUNKS):
                dst = xg.at[op, pl.ds(src * sub + h * piece, piece)]
                pltpu.make_async_copy(dst, dst, p_rs.at[op, src, h]).wait()

    def spread_sent(op):
        for slot in range(rows):
            for h in range(CHUNKS):
                @pl.when((slot <= z) & (z < rows - 1))
                def _():
                    z_copy(op, slot, h, 1).wait_send()

                @pl.when((slot >= z) & (z > 0))
                def _():
                    z_copy(op, slot, h, -1).wait_send()

                @pl.when(slot != c)
                def _():
                    p_copy(op, slot, h).wait_send()

    def core_copy(op, yy):
        return rcopy(part.at[op, 2 * yy + 1 - k], rsa.at[op, yy], rsa_ss.at[op, yy], rsa_rs.at[op, yy], partner)

    def y_copy(op):
        return rcopy(sb.at[op], rsb.at[op], rsb_ss.at[op], rsb_rs.at[op], across)

    def product(op):
        def step(i, carry):
            yy = (1 - y) + (i // 2) * (2 * y - 1)
            kk = (1 - k) + lax.rem(i, 2) * (2 * k - 1)
            j = 2 * yy + kk
            part[op, j] = dot(a_v[op, pl.ds(pl.multiple_of(j * sub, sub), sub), :], xg[op], 1, 0)

            @pl.when(lax.rem(i, 2) == 0)
            def _():
                core_copy(op, yy).start()

            @pl.when(i == 1)
            def _():
                core_copy(op, 1 - y).wait_recv()
                sb[op] = part[op, j] + rsa[op, 1 - y]
                y_copy(op).start()

            return carry

        lax.fori_loop(0, col, step, 0)

    def product_end(op):
        core_copy(op, y).wait_recv()
        own = part[op, c] + rsa[op, y]
        y_copy(op).wait_recv()
        yv[op] = own + rsb[op]
        core_copy(op, 0).wait_send()
        core_copy(op, 1).wait_send()
        y_copy(op).wait_send()

    def c1(op):
        return rcopy(gp.at[op, pl.ds((1 - k) * half, half)], g1.at[op], g1_ss.at[op], g1_rs.at[op], partner)

    def c2(op):
        return rcopy(s1.at[op, pl.ds((1 - y) * quarter, quarter)], g2.at[op], g2_ss.at[op], g2_rs.at[op], across)

    chip, chips = 2 * z + y, 2 * rows

    def c3(op, turn, d, mine):
        other = lax.rem(chip + d, chips)
        at = chip if mine else other
        place = slots.at[op, turn, at]
        return rcopy(place, place, sl_ss.at[op, d], sl_rs.at[op, turn, at], dev(other // 2, lax.rem(other, 2), k))

    def c4(op):
        rng = pl.ds(k * half, half)
        return rcopy(gs.at[op, rng], gs.at[op, rng], g4_ss.at[op], g4_rs.at[op], partner)

    def c4_in(op):
        rng = pl.ds((1 - k) * half, half)
        return rcopy(gs.at[op, rng], gs.at[op, rng], g4_ss.at[op], g4_rs.at[op], partner)

    def sum_rest(ops, turn):
        for op in ops:
            c1(op).wait_recv()
            s1[op] = gp[op, pl.ds(pl.multiple_of(k * half, half), half), :] + g1[op]
            c2(op).start()
        for op in ops:
            c2(op).wait_recv()
            slots[op, turn, chip] = s1[op, pl.ds(pl.multiple_of(y * quarter, quarter), quarter), :] + g2[op]
            for d in range(1, chips):
                c3(op, turn, d, True).start()
        for op in ops:
            for d in range(1, chips):
                c3(op, turn, d, False).wait_recv()
            for yy in range(2):
                acc = slots[op, turn, yy]
                for zz in range(1, rows):
                    acc = acc + slots[op, turn, 2 * zz + yy]
                gs[op, pl.ds(pl.multiple_of(k * half + yy * quarter, quarter), quarter), :] = acc
            c4(op).start()
        for op in ops:
            c4_in(op).wait_recv()
            c1(op).wait_send()
            c2(op).wait_send()
            for d in range(1, chips):
                c3(op, turn, d, True).wait_send()
            c4(op).wait_send()

    lane = lax.broadcasted_iota(jnp.int32, (8, 128), 1)
    sublane = lax.broadcasted_iota(jnp.int32, (8, 128), 0)

    def factor(ops):
        eye = (lax.broadcasted_iota(jnp.int32, (128, 128), 0) == lax.broadcasted_iota(jnp.int32, (128, 128), 1)).astype(F32)
        for op in ops:
            gw[op, :, 0:128] = gs[op] / total
            gw[op, :, 128:256] = eye

        def step(i, carry):
            rng = pl.ds(pl.multiple_of(i * 8, 8), 8)
            for op in ops:
                p0, p1 = gw[op, rng, 0:128], gw[op, rng, 128:256]
                cols = []
                for j in range(8):
                    one = jnp.sum(jnp.where(lane == i * 8 + j, p0, 0.0), axis=1, keepdims=True)
                    cols.append(jnp.broadcast_to(one, (8, 128)))
                pivots = jnp.ones((8, 128), F32)
                for j in range(8):
                    d = jnp.broadcast_to(cols[j][j:j + 1], (8, 128))
                    pivots = jnp.where(sublane == j, d, pivots)
                    if j < 7:
                        m = jnp.where(sublane > j, cols[j] * (1.0 / d), 0.0)
                        p0 = p0 - m * jnp.broadcast_to(p0[j:j + 1], (8, 128))
                        p1 = p1 - m * jnp.broadcast_to(p1[j:j + 1], (8, 128))
                        for q in range(j + 1, 8):
                            cols[q] = cols[q] - m * jnp.broadcast_to(cols[q][j:j + 1], (8, 128))
                scale = lax.rsqrt(pivots)
                p0, p1 = p0 * scale, p1 * scale
                mv[op, rng, :] = p1
                l1, l2, l3 = split3(p0)
                r1, r2, r3 = split3(jnp.concatenate([p0, p1], axis=1))
                lhs = jnp.concatenate([l1, l1, l2, l1, l2, l3], axis=0).astype(BF16)
                rhs = jnp.concatenate([r1, r2, r1, r3, r2, r1], axis=0).astype(BF16)
                gw[op] = gw[op] - dot(lhs, rhs, 0, 0)
            return carry

        lax.fori_loop(0, 16, step, 0)

    for op in OPS:
        xz[op, z] = (left_start, right_start)[op][...].astype(BF16)
        spread_begin(op)
    for t in range(1, rows):
        for op in OPS:
            spread_step(op, t)
    for op in OPS:
        for j in range(col):
            load(op, j).wait()

    def products():
        for op in OPS:
            spread_end(op)
            product(op)
            spread_sent(op)

    def sweep(s, carry):
        products()
        for op in OPS:
            product_end(op)
            y_half = yv[op].astype(BF16)
            gp[op] = dot(y_half, y_half, 0, 0)
            c1(op).start()
        sum_rest(OPS, 0)
        factor(OPS)
        for op in OPS:
            y_one = dot(yv[op], mv[op], 1, 1, HIGHEST)
            yv[op] = y_one
            gp[op] = dot(y_one, y_one, 0, 0, HIGHEST)
            c1(op).start()
        sum_rest(OPS, 1)
        factor(OPS)
        for op in OPS:
            x = dot(yv[op], mv[op], 1, 1, HIGHEST)
            xf[op] = x
            xz[op, z] = x.astype(BF16)
            spread_begin(op)
        for t in range(1, rows):
            for op in OPS:
                spread_step(op, t)
        return carry

    lax.fori_loop(0, SWEEPS, sweep, 0)
    left_basis[...] = xf[0]
    right_basis[...] = xf[1]
    products()
    for op in OPS:
        product_end(op)
        gp[op] = dot(xf[op], yv[op], 0, 0, HIGHEST)
        c1(op).start()
    sum_rest(OPS, 0)
    left_ray[...] = gs[0] / total
    right_ray[...] = gs[1] / total


def solution(mesh):
    rows, col = mesh.shape["row"], mesh.shape["col"]

    def local_program(left_op, left_start, right_op, right_start):
        blk, s = left_op.shape[0], left_start.shape[1]
        sub = left_start.shape[0]
        vmem = pl.BlockSpec(memory_space=pltpu.VMEM)
        hbm = pl.BlockSpec(memory_space=pl.ANY)
        basis = jax.ShapeDtypeStruct((sub, s), F32)
        ray = jax.ShapeDtypeStruct((s, s), F32)
        dma = pltpu.SemaphoreType.DMA
        scratch = [
            pltpu.VMEM((2, blk, blk), BF16),
            pltpu.VMEM((2, blk, s), BF16),
            pltpu.VMEM((2, rows, sub, s), BF16),
            pltpu.VMEM((2, sub, s), F32),
            pltpu.VMEM((2, col, sub, s), F32),
            pltpu.VMEM((2, 2, sub, s), F32),
            pltpu.VMEM((2, sub, s), F32),
            pltpu.VMEM((2, sub, s), F32),
            pltpu.VMEM((2, sub, s), F32),
            pltpu.VMEM((2, s, s), F32),
            pltpu.VMEM((2, s // 2, s), F32),
            pltpu.VMEM((2, s // 2, s), F32),
            pltpu.VMEM((2, s // 4, s), F32),
            pltpu.VMEM((2, 2, 2 * rows, s // 4, s), F32),
            pltpu.VMEM((2, s, s), F32),
            pltpu.VMEM((2, s, 2 * s), F32),
            pltpu.VMEM((2, s, s), F32),
            dma((2, col)),
            dma((2, 2)), dma((2, 2)), dma((2,)), dma((2,)),
            dma((2,)), dma((2,)), dma((2,)), dma((2,)),
            dma((2, 2 * rows)), dma((2, 2, 2 * rows)), dma((2,)), dma((2,)),
            dma((2, rows, CHUNKS)), dma((2, rows, CHUNKS)), dma((2, rows, CHUNKS)),
            dma((2, rows, CHUNKS)), dma((2, col, CHUNKS)),
        ]
        return pl.pallas_call(
            functools.partial(kernel, rows, col),
            out_shape=(basis, ray, basis, ray),
            in_specs=[hbm, vmem, hbm, vmem],
            out_specs=(vmem,) * 4,
            scratch_shapes=scratch,
            compiler_params=pltpu.CompilerParams(collective_id=0, has_side_effects=True, vmem_limit_bytes=66_000_000),
        )(left_op, left_start, right_op, right_start)

    op_spec = P(("batch", "row"), "col")
    vec_spec = P(("batch", "row", "col"), None)
    small_spec = P("batch", None)
    return jax.shard_map(local_program, mesh=mesh, in_specs=(op_spec, vec_spec, op_spec, vec_spec), out_specs=(vec_spec, small_spec, vec_spec, small_spec), check_vma=False)
```

```python
import functools

import jax
import jax.numpy as jnp
from jax import lax
from jax.experimental import pallas as pl
from jax.experimental.pallas import tpu as pltpu
from jax.sharding import PartitionSpec as P

SWEEPS = 4
CHUNKS = 2
PARTS = 4
MESH = pl.DeviceIdType.MESH
HIGHEST = lax.Precision.HIGHEST
OPS = (0, 1)
F32 = jnp.float32
BF16 = jnp.bfloat16


def dot(lhs, rhs, lhs_dim, rhs_dim, precision=None):
    dims = (((lhs_dim,), (rhs_dim,)), ((), ()))
    return lax.dot_general(lhs, rhs, dims, precision=precision, preferred_element_type=F32)


def split3(v):
    one = v.astype(BF16).astype(F32)
    rest = v - one
    two = rest.astype(BF16).astype(F32)
    return one, two, rest - two


def kernel(rows, col, left_op, left_start, right_op, right_start, left_basis, left_ray, right_basis, right_ray,
           a_v, xg, xz, xf, part, rsa, sb, rsb, yv, gp, g1, s1, g2, slots, gs, gw, mv, keep,
           load_sem, rsa_ss, rsa_rs, rsb_ss, rsb_rs, g1_ss, g1_rs, g2_ss, g2_rs, sl_ss, sl_rs, g4_ss, g4_rs,
           zr_ss, zl_ss, z_rs, p_ss, p_rs):
    b, z, c = lax.axis_index("batch"), lax.axis_index("row"), lax.axis_index("col")
    y, k = c // 2, c % 2
    blk = a_v.shape[1]
    sub = blk // col
    piece = sub // CHUNKS
    total = blk * rows
    half, quarter = 64, 32

    def dev(zz, yy, kk):
        return (b, zz, 2 * yy + kk)

    def rcopy(src, dst, ss, rs, to):
        return pltpu.make_async_remote_copy(src_ref=src, dst_ref=dst, send_sem=ss, recv_sem=rs, device_id=to, device_id_type=MESH)

    partner, across = dev(z, y, 1 - k), dev(z, 1 - y, k)

    def load(op, j):
        src = (left_op, right_op)[op]
        rng = pl.ds(j * sub, sub)
        return pltpu.make_async_copy(src.at[rng], a_v.at[op, rng], load_sem.at[op, j])

    for op in OPS:
        for j in range(col):
            load(op, j).start()

    barrier = pltpu.get_barrier_semaphore()
    me = z * col + c
    count = rows * col
    for d in range(1, count):
        peer = lax.rem(me + d, count)
        pl.semaphore_signal(barrier, inc=1, device_id=(b, peer // col, lax.rem(peer, col)), device_id_type=MESH)
    pl.semaphore_wait(barrier, count - 1)

    def z_copy(op, slot, h, step):
        rng = pl.ds(h * piece, piece)
        to, ss = (dev(z + 1, y, k), zr_ss) if step > 0 else (dev(z - 1, y, k), zl_ss)
        return rcopy(xz.at[op, slot, rng], xz.at[op, slot, rng], ss.at[op, slot, h], z_rs.at[op, slot, h], to)

    def p_copy(op, slot, h):
        src = xz.at[op, slot, pl.ds(h * piece, piece)]
        dst = xg.at[op, pl.ds(c * sub + h * piece, piece)]
        return rcopy(src, dst, p_ss.at[op, slot, h], p_rs.at[op, c, h], dev(z, slot // 2, lax.rem(slot, 2)))

    def p_local(op, slot, h):
        src = xz.at[op, slot, pl.ds(h * piece, piece)]
        dst = xg.at[op, pl.ds(c * sub + h * piece, piece)]
        return pltpu.make_async_copy(src, dst, p_rs.at[op, c, h])

    def p_start(op, slot, h):
        @pl.when(slot == c)
        def _():
            p_local(op, slot, h).start()

        @pl.when(slot != c)
        def _():
            p_copy(op, slot, h).start()

    def spread_begin(op):
        for h in range(CHUNKS):
            @pl.when(z < rows - 1)
            def _():
                z_copy(op, z, h, 1).start()

            @pl.when(z > 0)
            def _():
                z_copy(op, z, h, -1).start()
        for h in range(CHUNKS):
            p_start(op, z, h)

    def spread_step(op, t, h):
        @pl.when(z - t >= 0)
        def _():
            slot = z - t
            z_copy(op, slot, h, 1).wait_recv()

            @pl.when(z < rows - 1)
            def _():
                z_copy(op, slot, h, 1).start()

            p_start(op, slot, h)

        @pl.when(z + t < rows)
        def _():
            slot = z + t
            z_copy(op, slot, h, -1).wait_recv()

            @pl.when(z > 0)
            def _():
                z_copy(op, slot, h, -1).start()

            p_start(op, slot, h)

    def spread_end(op):
        for src in range(col):
            for h in range(CHUNKS):
                dst = xg.at[op, pl.ds(src * sub + h * piece, piece)]
                pltpu.make_async_copy(dst, dst, p_rs.at[op, src, h]).wait()

    def spread_sent(op):
        for slot in range(rows):
            for h in range(CHUNKS):
                @pl.when((slot <= z) & (z < rows - 1))
                def _():
                    z_copy(op, slot, h, 1).wait_send()

                @pl.when((slot >= z) & (z > 0))
                def _():
                    z_copy(op, slot, h, -1).wait_send()

                @pl.when(slot != c)
                def _():
                    p_copy(op, slot, h).wait_send()

    def core_copy(op, yy):
        return rcopy(part.at[op, 2 * yy + 1 - k], rsa.at[op, yy], rsa_ss.at[op, yy], rsa_rs.at[op, yy], partner)

    def y_copy(op):
        return rcopy(sb.at[op], rsb.at[op], rsb_ss.at[op], rsb_rs.at[op], across)

    def product(op, i):
        yy, kk = (1 - y, y)[i // 2], (1 - k, k)[i % 2]
        j = 2 * yy + kk
        part[op, j] = dot(a_v[op, pl.ds(pl.multiple_of(j * sub, sub), sub), :], xg[op], 1, 0)
        if i % 2 == 0:
            core_copy(op, yy).start()
        if i == 1:
            core_copy(op, yy).wait_recv()
            sb[op] = part[op, j] + rsa[op, yy]
            y_copy(op).start()

    def product_end(op):
        core_copy(op, y).wait_recv()
        own = part[op, c] + rsa[op, y]
        y_copy(op).wait_recv()
        yv[op] = own + rsb[op]
        core_copy(op, 0).wait_send()
        core_copy(op, 1).wait_send()
        y_copy(op).wait_send()

    def c1(op):
        return rcopy(gp.at[op, pl.ds((1 - k) * half, half)], g1.at[op], g1_ss.at[op], g1_rs.at[op], partner)

    def c2(op):
        return rcopy(s1.at[op, pl.ds((1 - y) * quarter, quarter)], g2.at[op], g2_ss.at[op], g2_rs.at[op], across)

    chip, chips = 2 * z + y, 2 * rows

    def c3(op, turn, d, mine):
        other = lax.rem(chip + d, chips)
        at = chip if mine else other
        place = slots.at[op, turn, at]
        return rcopy(place, place, sl_ss.at[op, d], sl_rs.at[op, turn, at], dev(other // 2, lax.rem(other, 2), k))

    def c4(op):
        rng = pl.ds(k * half, half)
        return rcopy(gs.at[op, rng], gs.at[op, rng], g4_ss.at[op], g4_rs.at[op], partner)

    def c4_in(op):
        rng = pl.ds((1 - k) * half, half)
        return rcopy(gs.at[op, rng], gs.at[op, rng], g4_ss.at[op], g4_rs.at[op], partner)

    def group_sum(op, turn):
        c1(op).start()
        yield
        c1(op).wait_recv()
        s1[op] = gp[op, pl.ds(pl.multiple_of(k * half, half), half), :] + g1[op]
        c2(op).start()
        yield
        c2(op).wait_recv()
        slots[op, turn, chip] = s1[op, pl.ds(pl.multiple_of(y * quarter, quarter), quarter), :] + g2[op]
        for d in range(1, chips):
            c3(op, turn, d, True).start()
        yield
        for d in range(1, chips):
            c3(op, turn, d, False).wait_recv()
        for yy in range(2):
            acc = slots[op, turn, yy]
            for zz in range(1, rows):
                acc = acc + slots[op, turn, 2 * zz + yy]
            gs[op, pl.ds(pl.multiple_of(k * half + yy * quarter, quarter), quarter), :] = acc
        c4(op).start()
        yield
        c4_in(op).wait_recv()
        c1(op).wait_send()
        c2(op).wait_send()
        for d in range(1, chips):
            c3(op, turn, d, True).wait_send()
        c4(op).wait_send()

    lane = lax.broadcasted_iota(jnp.int32, (8, 128), 1)
    sublane = lax.broadcasted_iota(jnp.int32, (8, 128), 0)

    def spread_row(v, j):
        return jnp.broadcast_to(v[j:j + 1], (8, 128))

    def panel(op, i, state):
        p0, p1, q0, q1 = state
        now = pl.ds(pl.multiple_of(i * 8, 8), 8)
        following = jnp.minimum(i + 1, 15) * 8
        cols = []
        for base in (i * 8, following):
            for j in range(8):
                one = jnp.sum(jnp.where(lane == base + j, p0, 0.0), axis=1, keepdims=True)
                cols.append(jnp.broadcast_to(one, (8, 128)))
        l1, l2, l3 = split3(q0)
        r1, r2, r3 = split3(jnp.concatenate([q0, q1], axis=1))
        lhs = jnp.concatenate([l1, l1, l2, l1, l2, l3], axis=0).astype(BF16)
        rhs = jnp.concatenate([r1, r2, r1, r3, r2, r1], axis=0).astype(BF16)
        gw[op] = gw[op] - dot(lhs, rhs, 0, 0)
        scale = jnp.ones((8, 128), F32)
        for j in range(8):
            root = lax.rsqrt(spread_row(cols[j], j))
            scale = jnp.where(sublane == j, root, scale)
            if j < 7:
                m = jnp.where(sublane > j, cols[j] * (root * root), 0.0)
                for q in range(j + 1, 16):
                    cols[q] = cols[q] - m * spread_row(cols[q], j)
                p0 = p0 - m * spread_row(p0, j)
                p1 = p1 - m * spread_row(p1, j)
        p0, p1 = p0 * scale, p1 * scale
        mv[op, now, :] = p1
        s0, s1_ = jnp.zeros((8, 128), F32), jnp.zeros((8, 128), F32)
        for j in range(8):
            w = cols[8 + j] * scale
            s0 = jnp.where(sublane == j, jnp.sum(w * p0, axis=0, keepdims=True), s0)
            s1_ = jnp.where(sublane == j, jnp.sum(w * p1, axis=0, keepdims=True), s1_)
        rng = pl.ds(pl.multiple_of(following, 8), 8)
        return gw[op, rng, 0:128] - s0, gw[op, rng, 128:256] - s1_, p0, p1

    def factor(op):
        eye = (lax.broadcasted_iota(jnp.int32, (128, 128), 0) == lax.broadcasted_iota(jnp.int32, (128, 128), 1)).astype(F32)
        g = gs[op] / total
        gw[op, :, 0:128] = g
        gw[op, :, 128:256] = eye
        zero = jnp.zeros((8, 128), F32)
        state = (g[0:8], eye[0:8], zero, zero)
        for part_no in range(PARTS):
            if part_no:
                yield
                state = tuple(keep[op, i] for i in range(4))
            n = 16 // PARTS
            state = lax.fori_loop(n * part_no, n * part_no + n, lambda i, st: panel(op, i, st), state)
            if part_no < PARTS - 1:
                for i in range(4):
                    keep[op, i] = state[i]

    def transport(op, first=False):
        spread_begin(op)
        yield
        for t in range(1, rows):
            for h in range(CHUNKS):
                spread_step(op, t, h)
                yield
        if first:
            for j in range(col):
                load(op, j).wait()
        spread_end(op)
        for i in range(4):
            product(op, i)
            yield
        spread_sent(op)
        product_end(op)

    def ortho(op):
        y_half = yv[op].astype(BF16)
        gp[op] = dot(y_half, y_half, 0, 0)
        yield from group_sum(op, 0)
        yield from factor(op)
        yield
        y_one = dot(yv[op], mv[op], 1, 1, HIGHEST)
        yv[op] = y_one
        gp[op] = dot(y_one, y_one, 0, 0, HIGHEST)
        yield from group_sum(op, 1)
        yield from factor(op)
        x = dot(yv[op], mv[op], 1, 1, HIGHEST)
        xf[op] = x
        xz[op, z] = x.astype(BF16)

    def rayleigh(op):
        gp[op] = dot(xf[op], yv[op], 0, 0, HIGHEST)
        yield from group_sum(op, 0)
        (left_ray, right_ray)[op][...] = gs[op] / total

    def run(order, **streams):
        for name in order:
            next(streams[name], None)
        for stream in streams.values():
            for _ in stream:
                pass

    ORDER = "TOOOTTTTOOTOOTOOTOTTOTOOOOO"
    xz[0, z] = left_start[...].astype(BF16)
    xz[1, z] = right_start[...].astype(BF16)
    run("", T=transport(0, True))
    for j in range(col):
        load(1, j).wait()

    def sweep(s, carry):
        run(ORDER, O=ortho(0), T=transport(1))
        run(ORDER, O=ortho(1), T=transport(0))
        return carry

    lax.fori_loop(0, SWEEPS, sweep, 0)
    left_basis[...] = xf[0]
    right_basis[...] = xf[1]
    run("TOOOTTTTOO", O=rayleigh(0), T=transport(1))
    run("", O=rayleigh(1))


def solution(mesh):
    rows, col = mesh.shape["row"], mesh.shape["col"]

    def local_program(left_op, left_start, right_op, right_start):
        blk, s = left_op.shape[0], left_start.shape[1]
        sub = left_start.shape[0]
        vmem = pl.BlockSpec(memory_space=pltpu.VMEM)
        hbm = pl.BlockSpec(memory_space=pl.ANY)
        basis = jax.ShapeDtypeStruct((sub, s), F32)
        ray = jax.ShapeDtypeStruct((s, s), F32)
        dma = pltpu.SemaphoreType.DMA
        scratch = [
            pltpu.VMEM((2, blk, blk), BF16),
            pltpu.VMEM((2, blk, s), BF16),
            pltpu.VMEM((2, rows, sub, s), BF16),
            pltpu.VMEM((2, sub, s), F32),
            pltpu.VMEM((2, col, sub, s), F32),
            pltpu.VMEM((2, 2, sub, s), F32),
            pltpu.VMEM((2, sub, s), F32),
            pltpu.VMEM((2, sub, s), F32),
            pltpu.VMEM((2, sub, s), F32),
            pltpu.VMEM((2, s, s), F32),
            pltpu.VMEM((2, s // 2, s), F32),
            pltpu.VMEM((2, s // 2, s), F32),
            pltpu.VMEM((2, s // 4, s), F32),
            pltpu.VMEM((2, 2, 2 * rows, s // 4, s), F32),
            pltpu.VMEM((2, s, s), F32),
            pltpu.VMEM((2, s, 2 * s), F32),
            pltpu.VMEM((2, s, s), F32),
            pltpu.VMEM((2, 4, 8, s), F32),
            dma((2, col)),
            dma((2, 2)), dma((2, 2)), dma((2,)), dma((2,)),
            dma((2,)), dma((2,)), dma((2,)), dma((2,)),
            dma((2, 2 * rows)), dma((2, 2, 2 * rows)), dma((2,)), dma((2,)),
            dma((2, rows, CHUNKS)), dma((2, rows, CHUNKS)), dma((2, rows, CHUNKS)),
            dma((2, rows, CHUNKS)), dma((2, col, CHUNKS)),
        ]
        return pl.pallas_call(
            functools.partial(kernel, rows, col),
            out_shape=(basis, ray, basis, ray),
            in_specs=[hbm, vmem, hbm, vmem],
            out_specs=(vmem,) * 4,
            scratch_shapes=scratch,
            compiler_params=pltpu.CompilerParams(collective_id=0, has_side_effects=True, vmem_limit_bytes=66_000_000),
        )(left_op, left_start, right_op, right_start)

    op_spec = P(("batch", "row"), "col")
    vec_spec = P(("batch", "row", "col"), None)
    small_spec = P("batch", None)
    return jax.shard_map(local_program, mesh=mesh, in_specs=(op_spec, vec_spec, op_spec, vec_spec), out_specs=(vec_spec, small_spec, vec_spec, small_spec), check_vma=False)
```

```python
import functools

import jax
import jax.numpy as jnp
from jax import lax
from jax.experimental import pallas as pl
from jax.experimental.pallas import tpu as pltpu
from jax.sharding import PartitionSpec as P

SWEEPS = 4
CHUNKS = 2
PARTS = 4
MESH = pl.DeviceIdType.MESH
HIGHEST = lax.Precision.HIGHEST
OPS = (0, 1)
F32 = jnp.float32
BF16 = jnp.bfloat16


def dot(lhs, rhs, lhs_dim, rhs_dim, precision=None):
    dims = (((lhs_dim,), (rhs_dim,)), ((), ()))
    return lax.dot_general(lhs, rhs, dims, precision=precision, preferred_element_type=F32)


def split3(v):
    one = v.astype(BF16).astype(F32)
    rest = v - one
    two = rest.astype(BF16).astype(F32)
    return one, two, rest - two


def kernel(rows, col, left_op, left_start, right_op, right_start, left_basis, left_ray, right_basis, right_ray,
           a_v, xg, xz, xf, part, rsa, sb, rsb, yv, gp, g1, s1, g2, slots, gs, gw, mv, keep,
           load_sem, rsa_ss, rsa_rs, rsb_ss, rsb_rs, g1_ss, g1_rs, g2_ss, g2_rs, sl_ss, sl_rs, g4_ss, g4_rs,
           zr_ss, zl_ss, z_rs, p_ss, p_rs):
    b, z, c = lax.axis_index("batch"), lax.axis_index("row"), lax.axis_index("col")
    y, k = c // 2, c % 2
    blk = a_v.shape[1]
    sub = blk // col
    piece = sub // CHUNKS
    total = blk * rows

    def dev(zz, yy, kk):
        return (b, zz, 2 * yy + kk)

    def rcopy(src, dst, ss, rs, to):
        return pltpu.make_async_remote_copy(src_ref=src, dst_ref=dst, send_sem=ss, recv_sem=rs, device_id=to, device_id_type=MESH)

    partner, across = dev(z, y, 1 - k), dev(z, 1 - y, k)

    def load(op, j):
        src = (left_op, right_op)[op]
        rng = pl.ds(j * sub, sub)
        return pltpu.make_async_copy(src.at[rng], a_v.at[op, rng], load_sem.at[op, j])

    for op in OPS:
        for j in range(col):
            load(op, j).start()

    barrier = pltpu.get_barrier_semaphore()
    me = z * col + c
    count = rows * col
    for d in range(1, count):
        peer = lax.rem(me + d, count)
        pl.semaphore_signal(barrier, inc=1, device_id=(b, peer // col, lax.rem(peer, col)), device_id_type=MESH)
    pl.semaphore_wait(barrier, count - 1)

    def z_copy(op, slot, h, step):
        rng = pl.ds(h * piece, piece)
        to, ss = (dev(z + 1, y, k), zr_ss) if step > 0 else (dev(z - 1, y, k), zl_ss)
        return rcopy(xz.at[op, slot, rng], xz.at[op, slot, rng], ss.at[op, slot, h], z_rs.at[op, slot, h], to)

    def p_copy(op, slot, h):
        src = xz.at[op, slot, pl.ds(h * piece, piece)]
        dst = xg.at[op, pl.ds(c * sub + h * piece, piece)]
        return rcopy(src, dst, p_ss.at[op, slot, h], p_rs.at[op, c, h], dev(z, slot // 2, lax.rem(slot, 2)))

    def p_local(op, slot, h):
        src = xz.at[op, slot, pl.ds(h * piece, piece)]
        dst = xg.at[op, pl.ds(c * sub + h * piece, piece)]
        return pltpu.make_async_copy(src, dst, p_rs.at[op, c, h])

    def p_start(op, slot, h):
        @pl.when(slot == c)
        def _():
            p_local(op, slot, h).start()

        @pl.when(slot != c)
        def _():
            p_copy(op, slot, h).start()

    def spread_begin(op):
        for h in range(CHUNKS):
            @pl.when(z < rows - 1)
            def _():
                z_copy(op, z, h, 1).start()

            @pl.when(z > 0)
            def _():
                z_copy(op, z, h, -1).start()
        for h in range(CHUNKS):
            p_start(op, z, h)

    def spread_step(op, t, h):
        @pl.when(z - t >= 0)
        def _():
            slot = z - t
            z_copy(op, slot, h, 1).wait_recv()

            @pl.when(z < rows - 1)
            def _():
                z_copy(op, slot, h, 1).start()

            p_start(op, slot, h)

        @pl.when(z + t < rows)
        def _():
            slot = z + t
            z_copy(op, slot, h, -1).wait_recv()

            @pl.when(z > 0)
            def _():
                z_copy(op, slot, h, -1).start()

            p_start(op, slot, h)

    def spread_end(op):
        for src in range(col):
            for h in range(CHUNKS):
                dst = xg.at[op, pl.ds(src * sub + h * piece, piece)]
                pltpu.make_async_copy(dst, dst, p_rs.at[op, src, h]).wait()

    def spread_sent(op):
        for slot in range(rows):
            for h in range(CHUNKS):
                @pl.when((slot <= z) & (z < rows - 1))
                def _():
                    z_copy(op, slot, h, 1).wait_send()

                @pl.when((slot >= z) & (z > 0))
                def _():
                    z_copy(op, slot, h, -1).wait_send()

                @pl.when(slot != c)
                def _():
                    p_copy(op, slot, h).wait_send()

    def core_copy(op, yy):
        return rcopy(part.at[op, 2 * yy + 1 - k], rsa.at[op, yy], rsa_ss.at[op, yy], rsa_rs.at[op, yy], partner)

    def y_copy(op):
        return rcopy(sb.at[op], rsb.at[op], rsb_ss.at[op], rsb_rs.at[op], across)

    def product(op, i):
        yy, kk = (1 - y, y)[i // 2], (1 - k, k)[i % 2]
        j = 2 * yy + kk
        part[op, j] = dot(a_v[op, pl.ds(pl.multiple_of(j * sub, sub), sub), :], xg[op], 1, 0)
        if i % 2 == 0:
            core_copy(op, yy).start()
        if i == 1:
            core_copy(op, yy).wait_recv()
            sb[op] = part[op, j] + rsa[op, yy]
            y_copy(op).start()

    def product_end(op):
        core_copy(op, y).wait_recv()
        own = part[op, c] + rsa[op, y]
        y_copy(op).wait_recv()
        yv[op] = own + rsb[op]
        core_copy(op, 0).wait_send()
        core_copy(op, 1).wait_send()
        y_copy(op).wait_send()

    def group_sum(op, turn, size):
        half, quarter = size // 2, size // 4

        def rng(which, length):
            return pl.ds(pl.multiple_of(which * length, length), length)

        c1 = rcopy(gp.at[op, rng(1 - k, half)], g1.at[op, pl.ds(0, half)], g1_ss.at[op], g1_rs.at[op], partner)
        c2 = rcopy(s1.at[op, rng(1 - y, quarter)], g2.at[op, pl.ds(0, quarter)], g2_ss.at[op], g2_rs.at[op], across)
        c4 = rcopy(gs.at[op, rng(k, half)], gs.at[op, rng(k, half)], g4_ss.at[op], g4_rs.at[op], partner)
        c4_in = rcopy(gs.at[op, rng(1 - k, half)], gs.at[op, rng(1 - k, half)], g4_ss.at[op], g4_rs.at[op], partner)
        chip, chips = 2 * z + y, 2 * rows

        def c3(d, mine):
            other = lax.rem(chip + d, chips)
            at = chip if mine else other
            place = slots.at[op, turn, at, pl.ds(0, quarter)]
            return rcopy(place, place, sl_ss.at[op, d], sl_rs.at[op, turn, at], dev(other // 2, lax.rem(other, 2), k))

        def over_cores():
            c1.wait_recv()
            s1[op, 0:half] = gp[op, rng(k, half), :] + g1[op, 0:half]
            c2.start()

        def over_y():
            c2.wait_recv()
            slots[op, turn, chip, 0:quarter] = s1[op, rng(y, quarter), :] + g2[op, 0:quarter]
            for d in range(1, chips):
                c3(d, True).start()

        def over_chips():
            for d in range(1, chips):
                c3(d, False).wait_recv()
            for yy in range(2):
                acc = slots[op, turn, yy, 0:quarter]
                for zz in range(1, rows):
                    acc = acc + slots[op, turn, 2 * zz + yy, 0:quarter]
                gs[op, pl.ds(pl.multiple_of(k * half + yy * quarter, quarter), quarter), :] = acc
            c4.start()

        def finish():
            c4_in.wait_recv()
            c1.wait_send()
            c2.wait_send()
            for d in range(1, chips):
                c3(d, True).wait_send()
            c4.wait_send()

        return c1.start, over_cores, over_y, over_chips, finish

    lane = lax.broadcasted_iota(jnp.int32, (8, 128), 1)
    sublane = lax.broadcasted_iota(jnp.int32, (8, 128), 0)

    def spread_row(v, j):
        return jnp.broadcast_to(v[j:j + 1], (8, 128))

    def panel(op, i, state):
        p0, p1, q0, q1 = state
        now = pl.ds(pl.multiple_of(i * 8, 8), 8)
        following = jnp.minimum(i + 1, 15) * 8
        cols = []
        for base in (i * 8, following):
            for j in range(8):
                one = jnp.sum(jnp.where(lane == base + j, p0, 0.0), axis=1, keepdims=True)
                cols.append(jnp.broadcast_to(one, (8, 128)))
        l1, l2, l3 = split3(q0)
        r1, r2, r3 = split3(jnp.concatenate([q0, q1], axis=1))
        lhs = jnp.concatenate([l1, l1, l2, l1, l2, l3], axis=0).astype(BF16)
        rhs = jnp.concatenate([r1, r2, r1, r3, r2, r1], axis=0).astype(BF16)
        gw[op] = gw[op] - dot(lhs, rhs, 0, 0)
        scale = jnp.ones((8, 128), F32)
        for j in range(8):
            root = lax.rsqrt(spread_row(cols[j], j))
            scale = jnp.where(sublane == j, root, scale)
            if j < 7:
                m = jnp.where(sublane > j, cols[j] * (root * root), 0.0)
                for q in range(j + 1, 16):
                    cols[q] = cols[q] - m * spread_row(cols[q], j)
                p0 = p0 - m * spread_row(p0, j)
                p1 = p1 - m * spread_row(p1, j)
        p0, p1 = p0 * scale, p1 * scale
        mv[op, now, :] = p1
        s0, s1_ = jnp.zeros((8, 128), F32), jnp.zeros((8, 128), F32)
        for j in range(8):
            w = cols[8 + j] * scale
            s0 = jnp.where(sublane == j, jnp.sum(w * p0, axis=0, keepdims=True), s0)
            s1_ = jnp.where(sublane == j, jnp.sum(w * p1, axis=0, keepdims=True), s1_)
        rng = pl.ds(pl.multiple_of(following, 8), 8)
        return gw[op, rng, 0:128] - s0, gw[op, rng, 128:256] - s1_, p0, p1

    def factor(op):
        zero = jnp.zeros((8, 128), F32)
        state = (gw[op, 0:8, 0:128], gw[op, 0:8, 128:256], zero, zero)
        for part_no in range(PARTS):
            if part_no:
                yield
                state = tuple(keep[op, i] for i in range(4))
            n = 16 // PARTS
            state = lax.fori_loop(n * part_no, n * part_no + n, lambda i, st: panel(op, i, st), state)
            if part_no < PARTS - 1:
                for i in range(4):
                    keep[op, i] = state[i]

    def eye():
        return (lax.broadcasted_iota(jnp.int32, (128, 128), 0) == lax.broadcasted_iota(jnp.int32, (128, 128), 1)).astype(F32)

    def transport(op, done, first=False):
        for n in range(done, (rows - 1) * CHUNKS):
            spread_step(op, n // CHUNKS + 1, n % CHUNKS)
            yield
        if first:
            for j in range(col):
                load(op, j).wait()
        spread_end(op)
        for i in range(4):
            product(op, i)
            yield
        spread_sent(op)
        product_end(op)

    def ortho(op, last):
        y_cur = yv[op]
        y_half = y_cur.astype(BF16)
        gp[op, 0:128] = dot(y_half, y_half, 0, 0)
        gp[op, 128:256] = dot(y_cur, y_cur, 0, 0, HIGHEST)
        steps = group_sum(op, 0, 256)
        steps[0]()
        for step in steps[1:-1]:
            yield
            step()
        yield
        steps[-1]()
        gw[op, :, 0:128] = gs[op, 0:128] / total
        gw[op, :, 128:256] = eye()
        yield from factor(op)
        yield
        steps = group_sum(op, 1, 128)

        @pl.when(last)
        def _():
            y_one = dot(yv[op], mv[op], 1, 1, HIGHEST)
            yv[op] = y_one
            gp[op, 0:128] = dot(y_one, y_one, 0, 0, HIGHEST)
            steps[0]()

        @pl.when(jnp.logical_not(last))
        def _():
            inv = mv[op]
            gw[op, :, 0:128] = dot(dot(inv, gs[op, 128:256] / total, 1, 0, HIGHEST), inv, 1, 1, HIGHEST)
            gw[op, :, 128:256] = inv

        for step in steps[1:-1]:
            yield
            pl.when(last)(step)
        yield

        @pl.when(last)
        def _():
            steps[-1]()
            gw[op, :, 0:128] = gs[op, 0:128] / total
            gw[op, :, 128:256] = eye()

        yield from factor(op)
        x = dot(yv[op], mv[op], 1, 1, HIGHEST)
        xf[op] = x
        xz[op, z] = x.astype(BF16)
        spread_begin(op)

    def rayleigh(op):
        gp[op, 0:128] = dot(xf[op], yv[op], 0, 0, HIGHEST)
        steps = group_sum(op, 0, 128)
        steps[0]()
        for step in steps[1:]:
            yield
            step()
        (left_ray, right_ray)[op][...] = gs[op, 0:128] / total

    def run(order, **streams):
        for name in order:
            next(streams[name], None)

    def rest(stream):
        for _ in stream:
            pass

    def half_sweep(o_op, t_op, last):
        o, t = ortho(o_op, last), transport(t_op, 1)
        run("OTOTOTTTOTTOTTOOOOOOO", O=o, T=t)
        rest(o)
        spread_step(o_op, 1, 0)
        rest(t)

    xz[0, z] = left_start[...].astype(BF16)
    spread_begin(0)
    xz[1, z] = right_start[...].astype(BF16)
    t = transport(0, 0, True)
    run("T" * ((rows - 1) * CHUNKS), T=t)
    spread_begin(1)
    run("TTTT", T=t)
    spread_step(1, 1, 0)
    rest(t)
    for j in range(col):
        load(1, j).wait()

    def sweep(s, carry):
        half_sweep(0, 1, s == SWEEPS - 1)
        half_sweep(1, 0, s == SWEEPS - 1)
        return carry

    lax.fori_loop(0, SWEEPS, sweep, 0)
    left_basis[...] = xf[0]
    right_basis[...] = xf[1]
    o, t = rayleigh(0), transport(1, 1)
    run("OTOTOTTTOO", O=o, T=t)
    rest(t)
    rest(o)
    rest(rayleigh(1))


def solution(mesh):
    rows, col = mesh.shape["row"], mesh.shape["col"]

    def local_program(left_op, left_start, right_op, right_start):
        blk, s = left_op.shape[0], left_start.shape[1]
        sub = left_start.shape[0]
        vmem = pl.BlockSpec(memory_space=pltpu.VMEM)
        hbm = pl.BlockSpec(memory_space=pl.ANY)
        basis = jax.ShapeDtypeStruct((sub, s), F32)
        ray = jax.ShapeDtypeStruct((s, s), F32)
        dma = pltpu.SemaphoreType.DMA
        scratch = [
            pltpu.VMEM((2, blk, blk), BF16),
            pltpu.VMEM((2, blk, s), BF16),
            pltpu.VMEM((2, rows, sub, s), BF16),
            pltpu.VMEM((2, sub, s), F32),
            pltpu.VMEM((2, col, sub, s), F32),
            pltpu.VMEM((2, 2, sub, s), F32),
            pltpu.VMEM((2, sub, s), F32),
            pltpu.VMEM((2, sub, s), F32),
            pltpu.VMEM((2, sub, s), F32),
            pltpu.VMEM((2, 2 * s, s), F32),
            pltpu.VMEM((2, s, s), F32),
            pltpu.VMEM((2, s, s), F32),
            pltpu.VMEM((2, s // 2, s), F32),
            pltpu.VMEM((2, 2, 2 * rows, s // 2, s), F32),
            pltpu.VMEM((2, 2 * s, s), F32),
            pltpu.VMEM((2, s, 2 * s), F32),
            pltpu.VMEM((2, s, s), F32),
            pltpu.VMEM((2, 4, 8, s), F32),
            dma((2, col)),
            dma((2, 2)), dma((2, 2)), dma((2,)), dma((2,)),
            dma((2,)), dma((2,)), dma((2,)), dma((2,)),
            dma((2, 2 * rows)), dma((2, 2, 2 * rows)), dma((2,)), dma((2,)),
            dma((2, rows, CHUNKS)), dma((2, rows, CHUNKS)), dma((2, rows, CHUNKS)),
            dma((2, rows, CHUNKS)), dma((2, col, CHUNKS)),
        ]
        return pl.pallas_call(
            functools.partial(kernel, rows, col),
            out_shape=(basis, ray, basis, ray),
            in_specs=[hbm, vmem, hbm, vmem],
            out_specs=(vmem,) * 4,
            scratch_shapes=scratch,
            compiler_params=pltpu.CompilerParams(collective_id=0, has_side_effects=True, vmem_limit_bytes=66_000_000),
        )(left_op, left_start, right_op, right_start)

    op_spec = P(("batch", "row"), "col")
    vec_spec = P(("batch", "row", "col"), None)
    small_spec = P("batch", None)
    return jax.shard_map(local_program, mesh=mesh, in_specs=(op_spec, vec_spec, op_spec, vec_spec), out_specs=(vec_spec, small_spec, vec_spec, small_spec), check_vma=False)
```

```python
import functools

import jax
import jax.numpy as jnp
from jax import lax
from jax.experimental import pallas as pl
from jax.experimental.pallas import tpu as pltpu
from jax.sharding import PartitionSpec as P

SWEEPS = 4
CHUNKS = 2
PARTS = 4
MESH = pl.DeviceIdType.MESH
HIGHEST = lax.Precision.HIGHEST
OPS = (0, 1)
F32 = jnp.float32
BF16 = jnp.bfloat16


def dot(lhs, rhs, lhs_dim, rhs_dim, precision=None):
    dims = (((lhs_dim,), (rhs_dim,)), ((), ()))
    return lax.dot_general(lhs, rhs, dims, precision=precision, preferred_element_type=F32)


def split3(v):
    one = v.astype(BF16).astype(F32)
    rest = v - one
    two = rest.astype(BF16).astype(F32)
    return one, two, rest - two


def kernel(rows, col, left_op, left_start, right_op, right_start, left_basis, left_ray, right_basis, right_ray,
           a_v, xg, xz, xf, part, rsa, sb, rsb, yv, gp, g1, s1, g2, slots, gs, gw, mv, keep,
           load_sem, rsa_ss, rsa_rs, rsb_ss, rsb_rs, g1_ss, g1_rs, g2_ss, g2_rs, sl_ss, sl_rs, g4_ss, g4_rs,
           zr_ss, zl_ss, z_rs, p_ss, p_rs):
    b, z, c = lax.axis_index("batch"), lax.axis_index("row"), lax.axis_index("col")
    y, k = c // 2, c % 2
    blk = a_v.shape[1]
    sub = blk // col
    piece = sub // CHUNKS
    total = blk * rows

    def dev(zz, yy, kk):
        return (b, zz, 2 * yy + kk)

    def rcopy(src, dst, ss, rs, to):
        return pltpu.make_async_remote_copy(src_ref=src, dst_ref=dst, send_sem=ss, recv_sem=rs, device_id=to, device_id_type=MESH)

    partner, across = dev(z, y, 1 - k), dev(z, 1 - y, k)

    def load(op, j):
        src = (left_op, right_op)[op]
        rng = pl.ds(j * sub, sub)
        return pltpu.make_async_copy(src.at[rng], a_v.at[op, rng], load_sem.at[op, j])

    for op in OPS:
        for j in range(col):
            load(op, j).start()

    barrier = pltpu.get_barrier_semaphore()
    me = z * col + c
    count = rows * col
    for d in range(1, count):
        peer = lax.rem(me + d, count)
        pl.semaphore_signal(barrier, inc=1, device_id=(b, peer // col, lax.rem(peer, col)), device_id_type=MESH)
    pl.semaphore_wait(barrier, count - 1)

    def z_copy(op, slot, h, step):
        rng = pl.ds(h * piece, piece)
        to, ss = (dev(z + 1, y, k), zr_ss) if step > 0 else (dev(z - 1, y, k), zl_ss)
        return rcopy(xz.at[op, slot, rng], xz.at[op, slot, rng], ss.at[op, slot, h], z_rs.at[op, slot, h], to)

    def p_copy(op, slot, h):
        src = xz.at[op, slot, pl.ds(h * piece, piece)]
        dst = xg.at[op, pl.ds(c * sub + h * piece, piece)]
        return rcopy(src, dst, p_ss.at[op, slot, h], p_rs.at[op, c, h], dev(z, slot // 2, lax.rem(slot, 2)))

    def p_local(op, slot, h):
        src = xz.at[op, slot, pl.ds(h * piece, piece)]
        dst = xg.at[op, pl.ds(c * sub + h * piece, piece)]
        return pltpu.make_async_copy(src, dst, p_rs.at[op, c, h])

    def p_start(op, slot, h):
        @pl.when(slot == c)
        def _():
            p_local(op, slot, h).start()

        @pl.when(slot != c)
        def _():
            p_copy(op, slot, h).start()

    def spread_begin(op):
        for h in range(CHUNKS):
            @pl.when(z < rows - 1)
            def _():
                z_copy(op, z, h, 1).start()

            @pl.when(z > 0)
            def _():
                z_copy(op, z, h, -1).start()
        for h in range(CHUNKS):
            p_start(op, z, h)

    def spread_step(op, t, h):
        @pl.when(z - t >= 0)
        def _():
            slot = z - t
            z_copy(op, slot, h, 1).wait_recv()

            @pl.when(z < rows - 1)
            def _():
                z_copy(op, slot, h, 1).start()

            p_start(op, slot, h)

        @pl.when(z + t < rows)
        def _():
            slot = z + t
            z_copy(op, slot, h, -1).wait_recv()

            @pl.when(z > 0)
            def _():
                z_copy(op, slot, h, -1).start()

            p_start(op, slot, h)

    def spread_end(op):
        for src in range(col):
            for h in range(CHUNKS):
                dst = xg.at[op, pl.ds(src * sub + h * piece, piece)]
                pltpu.make_async_copy(dst, dst, p_rs.at[op, src, h]).wait()

    def spread_sent(op):
        for slot in range(rows):
            for h in range(CHUNKS):
                @pl.when((slot <= z) & (z < rows - 1))
                def _():
                    z_copy(op, slot, h, 1).wait_send()

                @pl.when((slot >= z) & (z > 0))
                def _():
                    z_copy(op, slot, h, -1).wait_send()

                @pl.when(slot != c)
                def _():
                    p_copy(op, slot, h).wait_send()

    def core_copy(op, yy):
        return rcopy(part.at[op, 2 * yy + 1 - k], rsa.at[op, yy], rsa_ss.at[op, yy], rsa_rs.at[op, yy], partner)

    def y_copy(op):
        return rcopy(sb.at[op], rsb.at[op], rsb_ss.at[op], rsb_rs.at[op], across)

    def product(op, i):
        yy, kk = (1 - y, y)[i // 2], (1 - k, k)[i % 2]
        j = 2 * yy + kk
        part[op, j] = dot(a_v[op, pl.ds(pl.multiple_of(j * sub, sub), sub), :], xg[op], 1, 0)
        if i % 2 == 0:
            core_copy(op, yy).start()
        if i == 1:
            core_copy(op, yy).wait_recv()
            sb[op] = part[op, j] + rsa[op, yy]
            y_copy(op).start()

    def product_end(op):
        core_copy(op, y).wait_recv()
        own = part[op, c] + rsa[op, y]
        y_copy(op).wait_recv()
        yv[op] = own + rsb[op]
        core_copy(op, 0).wait_send()
        core_copy(op, 1).wait_send()
        y_copy(op).wait_send()

    def group_sum(op, turn, size):
        half, quarter = size // 2, size // 4

        def rng(which, length):
            return pl.ds(pl.multiple_of(which * length, length), length)

        c1 = rcopy(gp.at[op, rng(1 - k, half)], g1.at[op, pl.ds(0, half)], g1_ss.at[op], g1_rs.at[op], partner)
        c2 = rcopy(s1.at[op, rng(1 - y, quarter)], g2.at[op, pl.ds(0, quarter)], g2_ss.at[op], g2_rs.at[op], across)
        c4 = rcopy(gs.at[op, rng(k, half)], gs.at[op, rng(k, half)], g4_ss.at[op], g4_rs.at[op], partner)
        c4_in = rcopy(gs.at[op, rng(1 - k, half)], gs.at[op, rng(1 - k, half)], g4_ss.at[op], g4_rs.at[op], partner)
        chip, chips = 2 * z + y, 2 * rows

        def c3(d, mine):
            other = lax.rem(chip + d, chips)
            at = chip if mine else other
            place = slots.at[op, turn, at, pl.ds(0, quarter)]
            return rcopy(place, place, sl_ss.at[op, d], sl_rs.at[op, turn, at], dev(other // 2, lax.rem(other, 2), k))

        def over_cores():
            c1.wait_recv()
            s1[op, 0:half] = gp[op, rng(k, half), :] + g1[op, 0:half]
            c2.start()

        def over_y():
            c2.wait_recv()
            slots[op, turn, chip, 0:quarter] = s1[op, rng(y, quarter), :] + g2[op, 0:quarter]
            for d in range(1, chips):
                c3(d, True).start()

        def over_chips():
            for d in range(1, chips):
                c3(d, False).wait_recv()
            for yy in range(2):
                acc = slots[op, turn, yy, 0:quarter]
                for zz in range(1, rows):
                    acc = acc + slots[op, turn, 2 * zz + yy, 0:quarter]
                gs[op, pl.ds(pl.multiple_of(k * half + yy * quarter, quarter), quarter), :] = acc
            c4.start()

        def finish():
            c4_in.wait_recv()
            c1.wait_send()
            c2.wait_send()
            for d in range(1, chips):
                c3(d, True).wait_send()
            c4.wait_send()

        return c1.start, over_cores, over_y, over_chips, finish

    lane = lax.broadcasted_iota(jnp.int32, (8, 128), 1)
    sublane = lax.broadcasted_iota(jnp.int32, (8, 128), 0)

    def spread_row(v, j):
        return jnp.broadcast_to(v[j:j + 1], (8, 128))

    def panel(op, i, state):
        p0, p1, q0, q1 = state
        now = pl.ds(pl.multiple_of(i * 8, 8), 8)
        following = jnp.minimum(i + 1, 15) * 8
        cols = []
        for base in (i * 8, following):
            for j in range(8):
                one = jnp.sum(jnp.where(lane == base + j, p0, 0.0), axis=1, keepdims=True)
                cols.append(jnp.broadcast_to(one, (8, 128)))
        l1, l2, l3 = split3(q0)
        r1, r2, r3 = split3(jnp.concatenate([q0, q1], axis=1))
        lhs = jnp.concatenate([l1, l1, l2, l1, l2, l3], axis=0).astype(BF16)
        rhs = jnp.concatenate([r1, r2, r1, r3, r2, r1], axis=0).astype(BF16)
        gw[op] = gw[op] - dot(lhs, rhs, 0, 0)
        scale = jnp.ones((8, 128), F32)
        for j in range(8):
            root = lax.rsqrt(spread_row(cols[j], j))
            scale = jnp.where(sublane == j, root, scale)
            if j < 7:
                m = jnp.where(sublane > j, cols[j] * (root * root), 0.0)
                for q in range(j + 1, 16):
                    cols[q] = cols[q] - m * spread_row(cols[q], j)
                p0 = p0 - m * spread_row(p0, j)
                p1 = p1 - m * spread_row(p1, j)
        p0, p1 = p0 * scale, p1 * scale
        mv[op, now, :] = p1
        s0, s1_ = jnp.zeros((8, 128), F32), jnp.zeros((8, 128), F32)
        for j in range(8):
            w = cols[8 + j] * scale
            s0 = jnp.where(sublane == j, jnp.sum(w * p0, axis=0, keepdims=True), s0)
            s1_ = jnp.where(sublane == j, jnp.sum(w * p1, axis=0, keepdims=True), s1_)
        rng = pl.ds(pl.multiple_of(following, 8), 8)
        return gw[op, rng, 0:128] - s0, gw[op, rng, 128:256] - s1_, p0, p1

    def factor(op):
        zero = jnp.zeros((8, 128), F32)
        state = (gw[op, 0:8, 0:128], gw[op, 0:8, 128:256], zero, zero)
        for part_no in range(PARTS):
            if part_no:
                yield
                state = tuple(keep[op, i] for i in range(4))
            n = 16 // PARTS
            state = lax.fori_loop(n * part_no, n * part_no + n, lambda i, st: panel(op, i, st), state)
            if part_no < PARTS - 1:
                for i in range(4):
                    keep[op, i] = state[i]

    def eye():
        return (lax.broadcasted_iota(jnp.int32, (128, 128), 0) == lax.broadcasted_iota(jnp.int32, (128, 128), 1)).astype(F32)

    def transport(op, first=False):
        for n in range((rows - 1) * CHUNKS):
            spread_step(op, n // CHUNKS + 1, n % CHUNKS)
            yield
        if first:
            for j in range(col):
                load(op, j).wait()
        spread_end(op)
        for i in range(4):
            product(op, i)
            yield
        spread_sent(op)

    def ortho(op, last):
        product_end(op)
        y_cur = yv[op]
        y_half = y_cur.astype(BF16)
        gp[op, 0:128] = dot(y_half, y_half, 0, 0)
        gp[op, 128:256] = dot(y_cur, y_cur, 0, 0, HIGHEST)
        steps = group_sum(op, 0, 256)
        steps[0]()
        for step in steps[1:-1]:
            yield
            step()
        yield
        steps[-1]()
        gw[op, :, 0:128] = gs[op, 0:128] / total
        gw[op, :, 128:256] = eye()
        yield from factor(op)
        yield
        steps = group_sum(op, 1, 128)

        @pl.when(last)
        def _():
            y_one = dot(yv[op], mv[op], 1, 1, HIGHEST)
            yv[op] = y_one
            gp[op, 0:128] = dot(y_one, y_one, 0, 0, HIGHEST)
            steps[0]()

        @pl.when(jnp.logical_not(last))
        def _():
            inv = mv[op]
            gw[op, :, 0:128] = dot(dot(inv, gs[op, 128:256] / total, 1, 0, HIGHEST), inv, 1, 1, HIGHEST)
            gw[op, :, 128:256] = inv

        for step in steps[1:-1]:
            yield
            pl.when(last)(step)
        yield

        @pl.when(last)
        def _():
            steps[-1]()
            gw[op, :, 0:128] = gs[op, 0:128] / total
            gw[op, :, 128:256] = eye()

        yield from factor(op)
        x = dot(yv[op], mv[op], 1, 1, HIGHEST)
        xf[op] = x
        xz[op, z] = x.astype(BF16)
        spread_begin(op)

    def rayleigh(op):
        product_end(op)
        gp[op, 0:128] = dot(xf[op], yv[op], 0, 0, HIGHEST)
        steps = group_sum(op, 0, 128)
        steps[0]()
        for step in steps[1:]:
            yield
            step()
        (left_ray, right_ray)[op][...] = gs[op, 0:128] / total

    def run(order, **streams):
        for name in order:
            next(streams[name], None)

    def rest(stream):
        for _ in stream:
            pass

    def half_sweep(o_op, t_op, last):
        o, t = ortho(o_op, last), transport(t_op)
        run("OOTTOTTTOTOOTTOOOOTOTOOO", O=o, T=t)
        rest(t)
        rest(o)

    xz[0, z] = left_start[...].astype(BF16)
    spread_begin(0)
    xz[1, z] = right_start[...].astype(BF16)
    t = transport(0, True)
    run("T" * ((rows - 1) * CHUNKS), T=t)
    spread_begin(1)
    rest(t)
    for j in range(col):
        load(1, j).wait()

    def sweep(s, carry):
        half_sweep(0, 1, s == SWEEPS - 1)
        half_sweep(1, 0, s == SWEEPS - 1)
        return carry

    lax.fori_loop(0, SWEEPS, sweep, 0)
    left_basis[...] = xf[0]
    right_basis[...] = xf[1]
    o, t = rayleigh(0), transport(1)
    run("OOTTOTTTOTO", O=o, T=t)
    rest(t)
    rest(o)
    rest(rayleigh(1))


def solution(mesh):
    rows, col = mesh.shape["row"], mesh.shape["col"]

    def local_program(left_op, left_start, right_op, right_start):
        blk, s = left_op.shape[0], left_start.shape[1]
        sub = left_start.shape[0]
        vmem = pl.BlockSpec(memory_space=pltpu.VMEM)
        hbm = pl.BlockSpec(memory_space=pl.ANY)
        basis = jax.ShapeDtypeStruct((sub, s), F32)
        ray = jax.ShapeDtypeStruct((s, s), F32)
        dma = pltpu.SemaphoreType.DMA
        scratch = [
            pltpu.VMEM((2, blk, blk), BF16),
            pltpu.VMEM((2, blk, s), BF16),
            pltpu.VMEM((2, rows, sub, s), BF16),
            pltpu.VMEM((2, sub, s), F32),
            pltpu.VMEM((2, col, sub, s), F32),
            pltpu.VMEM((2, 2, sub, s), F32),
            pltpu.VMEM((2, sub, s), F32),
            pltpu.VMEM((2, sub, s), F32),
            pltpu.VMEM((2, sub, s), F32),
            pltpu.VMEM((2, 2 * s, s), F32),
            pltpu.VMEM((2, s, s), F32),
            pltpu.VMEM((2, s, s), F32),
            pltpu.VMEM((2, s // 2, s), F32),
            pltpu.VMEM((2, 2, 2 * rows, s // 2, s), F32),
            pltpu.VMEM((2, 2 * s, s), F32),
            pltpu.VMEM((2, s, 2 * s), F32),
            pltpu.VMEM((2, s, s), F32),
            pltpu.VMEM((2, 4, 8, s), F32),
            dma((2, col)),
            dma((2, 2)), dma((2, 2)), dma((2,)), dma((2,)),
            dma((2,)), dma((2,)), dma((2,)), dma((2,)),
            dma((2, 2 * rows)), dma((2, 2, 2 * rows)), dma((2,)), dma((2,)),
            dma((2, rows, CHUNKS)), dma((2, rows, CHUNKS)), dma((2, rows, CHUNKS)),
            dma((2, rows, CHUNKS)), dma((2, col, CHUNKS)),
        ]
        return pl.pallas_call(
            functools.partial(kernel, rows, col),
            out_shape=(basis, ray, basis, ray),
            in_specs=[hbm, vmem, hbm, vmem],
            out_specs=(vmem,) * 4,
            scratch_shapes=scratch,
            compiler_params=pltpu.CompilerParams(collective_id=0, has_side_effects=True, vmem_limit_bytes=66_000_000),
        )(left_op, left_start, right_op, right_start)

    op_spec = P(("batch", "row"), "col")
    vec_spec = P(("batch", "row", "col"), None)
    small_spec = P("batch", None)
    return jax.shard_map(local_program, mesh=mesh, in_specs=(op_spec, vec_spec, op_spec, vec_spec), out_specs=(vec_spec, small_spec, vec_spec, small_spec), check_vma=False)
```

```python
import functools

import jax
import jax.numpy as jnp
from jax import lax
from jax.experimental import pallas as pl
from jax.experimental.pallas import tpu as pltpu
from jax.sharding import PartitionSpec as P

SWEEPS = 4
CHUNKS = 2
PARTS = 4
MESH = pl.DeviceIdType.MESH
HIGHEST = lax.Precision.HIGHEST
OPS = (0, 1)
F32 = jnp.float32
BF16 = jnp.bfloat16


def dot(lhs, rhs, lhs_dim, rhs_dim, precision=None):
    dims = (((lhs_dim,), (rhs_dim,)), ((), ()))
    return lax.dot_general(lhs, rhs, dims, precision=precision, preferred_element_type=F32)


def split3(v):
    one = v.astype(BF16).astype(F32)
    rest = v - one
    two = rest.astype(BF16).astype(F32)
    return one, two, rest - two


def kernel(rows, col, left_op, left_start, right_op, right_start, left_basis, left_ray, right_basis, right_ray,
           a_v, xg, xz, xf, part, rsa, sb, rsb, yv, gp, g1, s1, g2, slots, gs, gw, mv, keep,
           load_sem, rsa_ss, rsa_rs, rsb_ss, rsb_rs, g1_ss, g1_rs, g2_ss, g2_rs, sl_ss, sl_rs, g4_ss, g4_rs,
           zr_ss, zl_ss, z_rs, p_ss, p_rs):
    b, z, c = lax.axis_index("batch"), lax.axis_index("row"), lax.axis_index("col")
    y, k = c // 2, c % 2
    blk = a_v.shape[1]
    sub = blk // col
    piece = sub // CHUNKS
    total = blk * rows

    def dev(zz, yy, kk):
        return (b, zz, 2 * yy + kk)

    def rcopy(src, dst, ss, rs, to):
        return pltpu.make_async_remote_copy(src_ref=src, dst_ref=dst, send_sem=ss, recv_sem=rs, device_id=to, device_id_type=MESH)

    partner, across = dev(z, y, 1 - k), dev(z, 1 - y, k)

    def load(op, j):
        src = (left_op, right_op)[op]
        rng = pl.ds(j * sub, sub)
        return pltpu.make_async_copy(src.at[rng], a_v.at[op, rng], load_sem.at[op, j])

    for op in OPS:
        for j in range(col):
            load(op, j).start()

    barrier = pltpu.get_barrier_semaphore()
    me = z * col + c
    count = rows * col
    for d in range(1, count):
        peer = lax.rem(me + d, count)
        pl.semaphore_signal(barrier, inc=1, device_id=(b, peer // col, lax.rem(peer, col)), device_id_type=MESH)
    pl.semaphore_wait(barrier, count - 1)

    def z_copy(op, slot, h, step):
        rng = pl.ds(h * piece, piece)
        to, ss = (dev(z + 1, y, k), zr_ss) if step > 0 else (dev(z - 1, y, k), zl_ss)
        return rcopy(xz.at[op, slot, rng], xz.at[op, slot, rng], ss.at[op, slot, h], z_rs.at[op, slot, h], to)

    def p_copy(op, slot, h):
        src = xz.at[op, slot, pl.ds(h * piece, piece)]
        dst = xg.at[op, pl.ds(c * sub + h * piece, piece)]
        return rcopy(src, dst, p_ss.at[op, slot, h], p_rs.at[op, c, h], dev(z, slot // 2, lax.rem(slot, 2)))

    def p_local(op, slot, h):
        src = xz.at[op, slot, pl.ds(h * piece, piece)]
        dst = xg.at[op, pl.ds(c * sub + h * piece, piece)]
        return pltpu.make_async_copy(src, dst, p_rs.at[op, c, h])

    def p_start(op, slot, h):
        @pl.when(slot == c)
        def _():
            p_local(op, slot, h).start()

        @pl.when(slot != c)
        def _():
            p_copy(op, slot, h).start()

    def spread_begin(op):
        for h in range(CHUNKS):
            @pl.when(z < rows - 1)
            def _():
                z_copy(op, z, h, 1).start()

            @pl.when(z > 0)
            def _():
                z_copy(op, z, h, -1).start()
        for h in range(CHUNKS):
            p_start(op, z, h)

    def spread_step(op, t, h):
        @pl.when(z - t >= 0)
        def _():
            slot = z - t
            z_copy(op, slot, h, 1).wait_recv()

            @pl.when(z < rows - 1)
            def _():
                z_copy(op, slot, h, 1).start()

            p_start(op, slot, h)

        @pl.when(z + t < rows)
        def _():
            slot = z + t
            z_copy(op, slot, h, -1).wait_recv()

            @pl.when(z > 0)
            def _():
                z_copy(op, slot, h, -1).start()

            p_start(op, slot, h)

    def spread_end(op):
        for src in range(col):
            for h in range(CHUNKS):
                dst = xg.at[op, pl.ds(src * sub + h * piece, piece)]
                pltpu.make_async_copy(dst, dst, p_rs.at[op, src, h]).wait()

    def spread_sent(op):
        for slot in range(rows):
            for h in range(CHUNKS):
                @pl.when((slot <= z) & (z < rows - 1))
                def _():
                    z_copy(op, slot, h, 1).wait_send()

                @pl.when((slot >= z) & (z > 0))
                def _():
                    z_copy(op, slot, h, -1).wait_send()

                @pl.when(slot != c)
                def _():
                    p_copy(op, slot, h).wait_send()

    def core_copy(op, yy):
        return rcopy(part.at[op, 2 * yy + 1 - k], rsa.at[op, yy], rsa_ss.at[op, yy], rsa_rs.at[op, yy], partner)

    def y_copy(op):
        return rcopy(sb.at[op], rsb.at[op], rsb_ss.at[op], rsb_rs.at[op], across)

    def product(op, i):
        yy, kk = (1 - y, y)[i // 2], (1 - k, k)[i % 2]
        j = 2 * yy + kk
        upper, lower = (
            dot(a_v[op, pl.ds(pl.multiple_of(j * sub + n * (sub // 2), sub // 2), sub // 2), :], xg[op], 1, 0) for n in range(2)
        )
        part[op, j, 0:sub // 2] = upper
        part[op, j, sub // 2:sub] = lower
        if i % 2 == 0:
            core_copy(op, yy).start()
        if i == 1:
            core_copy(op, yy).wait_recv()
            sb[op] = part[op, j] + rsa[op, yy]
            y_copy(op).start()

    def product_end(op):
        core_copy(op, y).wait_recv()
        own = part[op, c] + rsa[op, y]
        y_copy(op).wait_recv()
        yv[op] = own + rsb[op]
        core_copy(op, 0).wait_send()
        core_copy(op, 1).wait_send()
        y_copy(op).wait_send()

    def group_sum(op, turn, size):
        half, quarter = size // 2, size // 4

        def rng(which, length):
            return pl.ds(pl.multiple_of(which * length, length), length)

        c1 = rcopy(gp.at[op, rng(1 - k, half)], g1.at[op, pl.ds(0, half)], g1_ss.at[op], g1_rs.at[op], partner)
        c2 = rcopy(s1.at[op, rng(1 - y, quarter)], g2.at[op, pl.ds(0, quarter)], g2_ss.at[op], g2_rs.at[op], across)
        c4 = rcopy(gs.at[op, rng(k, half)], gs.at[op, rng(k, half)], g4_ss.at[op], g4_rs.at[op], partner)
        c4_in = rcopy(gs.at[op, rng(1 - k, half)], gs.at[op, rng(1 - k, half)], g4_ss.at[op], g4_rs.at[op], partner)
        chip, chips = 2 * z + y, 2 * rows

        def c3(d, mine):
            other = lax.rem(chip + d, chips)
            at = chip if mine else other
            place = slots.at[op, turn, at, pl.ds(0, quarter)]
            return rcopy(place, place, sl_ss.at[op, d], sl_rs.at[op, turn, at], dev(other // 2, lax.rem(other, 2), k))

        def over_cores():
            c1.wait_recv()
            s1[op, 0:half] = gp[op, rng(k, half), :] + g1[op, 0:half]
            c2.start()

        def over_y():
            c2.wait_recv()
            slots[op, turn, chip, 0:quarter] = s1[op, rng(y, quarter), :] + g2[op, 0:quarter]
            for d in range(1, chips):
                c3(d, True).start()

        def over_chips():
            for d in range(1, chips):
                c3(d, False).wait_recv()
            for yy in range(2):
                acc = slots[op, turn, yy, 0:quarter]
                for zz in range(1, rows):
                    acc = acc + slots[op, turn, 2 * zz + yy, 0:quarter]
                gs[op, pl.ds(pl.multiple_of(k * half + yy * quarter, quarter), quarter), :] = acc
            c4.start()

        def finish():
            c4_in.wait_recv()
            c1.wait_send()
            c2.wait_send()
            for d in range(1, chips):
                c3(d, True).wait_send()
            c4.wait_send()

        return c1.start, over_cores, over_y, over_chips, finish

    lane = lax.broadcasted_iota(jnp.int32, (8, 128), 1)
    sublane = lax.broadcasted_iota(jnp.int32, (8, 128), 0)

    def spread_row(v, j):
        return jnp.broadcast_to(v[j:j + 1], (8, 128))

    def panel(op, i, state):
        p0, p1, q0, q1 = state
        now = pl.ds(pl.multiple_of(i * 8, 8), 8)
        following = jnp.minimum(i + 1, 15) * 8
        cols = []
        for base in (i * 8, following):
            for j in range(8):
                one = jnp.sum(jnp.where(lane == base + j, p0, 0.0), axis=1, keepdims=True)
                cols.append(jnp.broadcast_to(one, (8, 128)))
        l1, l2, l3 = split3(q0)
        r1, r2, r3 = split3(jnp.concatenate([q0, q1], axis=1))
        lhs = jnp.concatenate([l1, l1, l2, l1, l2, l3], axis=0).astype(BF16)
        rhs = jnp.concatenate([r1, r2, r1, r3, r2, r1], axis=0).astype(BF16)
        gw[op] = gw[op] - dot(lhs, rhs, 0, 0)
        scale = jnp.ones((8, 128), F32)
        for j in range(8):
            root = lax.rsqrt(spread_row(cols[j], j))
            scale = jnp.where(sublane == j, root, scale)
            if j < 7:
                m = jnp.where(sublane > j, cols[j] * (root * root), 0.0)
                for q in range(j + 1, 16):
                    cols[q] = cols[q] - m * spread_row(cols[q], j)
                p0 = p0 - m * spread_row(p0, j)
                p1 = p1 - m * spread_row(p1, j)
        p0, p1 = p0 * scale, p1 * scale
        mv[op, now, :] = p1
        s0, s1_ = jnp.zeros((8, 128), F32), jnp.zeros((8, 128), F32)
        for j in range(8):
            w = cols[8 + j] * scale
            s0 = jnp.where(sublane == j, jnp.sum(w * p0, axis=0, keepdims=True), s0)
            s1_ = jnp.where(sublane == j, jnp.sum(w * p1, axis=0, keepdims=True), s1_)
        rng = pl.ds(pl.multiple_of(following, 8), 8)
        return gw[op, rng, 0:128] - s0, gw[op, rng, 128:256] - s1_, p0, p1

    def factor(op):
        zero = jnp.zeros((8, 128), F32)
        state = (gw[op, 0:8, 0:128], gw[op, 0:8, 128:256], zero, zero)
        for part_no in range(PARTS):
            if part_no:
                yield
                state = tuple(keep[op, i] for i in range(4))
            n = 16 // PARTS
            state = lax.fori_loop(n * part_no, n * part_no + n, lambda i, st: panel(op, i, st), state)
            if part_no < PARTS - 1:
                for i in range(4):
                    keep[op, i] = state[i]

    def eye():
        return (lax.broadcasted_iota(jnp.int32, (128, 128), 0) == lax.broadcasted_iota(jnp.int32, (128, 128), 1)).astype(F32)

    def transport(op, first=False):
        for n in range((rows - 1) * CHUNKS):
            spread_step(op, n // CHUNKS + 1, n % CHUNKS)
            yield
        if first:
            for j in range(col):
                load(op, j).wait()
        spread_end(op)
        for i in range(4):
            product(op, i)
            yield
        spread_sent(op)

    def ortho(op, last):
        product_end(op)
        y_cur = yv[op]
        y_half = y_cur.astype(BF16)
        gp[op, 0:128] = dot(y_half, y_half, 0, 0)
        gp[op, 128:256] = dot(y_cur, y_cur, 0, 0, HIGHEST)
        steps = group_sum(op, 0, 256)
        steps[0]()
        for step in steps[1:-1]:
            yield
            step()
        yield
        steps[-1]()
        gw[op, :, 0:128] = gs[op, 0:128] / total
        gw[op, :, 128:256] = eye()
        yield from factor(op)
        yield
        steps = group_sum(op, 1, 128)

        @pl.when(last)
        def _():
            y_one = dot(yv[op], mv[op], 1, 1, HIGHEST)
            yv[op] = y_one
            gp[op, 0:128] = dot(y_one, y_one, 0, 0, HIGHEST)
            steps[0]()

        @pl.when(jnp.logical_not(last))
        def _():
            inv = mv[op]
            gw[op, :, 0:128] = dot(dot(inv, gs[op, 128:256] / total, 1, 0, HIGHEST), inv, 1, 1, HIGHEST)
            gw[op, :, 128:256] = inv

        for step in steps[1:-1]:
            yield
            pl.when(last)(step)
        yield

        @pl.when(last)
        def _():
            steps[-1]()
            gw[op, :, 0:128] = gs[op, 0:128] / total
            gw[op, :, 128:256] = eye()

        yield from factor(op)
        x = dot(yv[op], mv[op], 1, 1, HIGHEST)
        xf[op] = x
        xz[op, z] = x.astype(BF16)
        spread_begin(op)

    def rayleigh(op):
        product_end(op)
        gp[op, 0:128] = dot(xf[op], yv[op], 0, 0, HIGHEST)
        steps = group_sum(op, 0, 128)
        steps[0]()
        for step in steps[1:]:
            yield
            step()
        (left_ray, right_ray)[op][...] = gs[op, 0:128] / total

    def run(order, **streams):
        for name in order:
            next(streams[name], None)

    def rest(stream):
        for _ in stream:
            pass

    def half_sweep(o_op, t_op, last):
        o, t = ortho(o_op, last), transport(t_op)
        run("OOTTOTTTOTOOTTOOOOTOTOOO", O=o, T=t)
        rest(t)
        rest(o)

    xz[0, z] = left_start[...].astype(BF16)
    spread_begin(0)
    xz[1, z] = right_start[...].astype(BF16)
    t = transport(0, True)
    run("T" * ((rows - 1) * CHUNKS), T=t)
    spread_begin(1)
    rest(t)
    for j in range(col):
        load(1, j).wait()

    def sweep(s, carry):
        half_sweep(0, 1, s == SWEEPS - 1)
        half_sweep(1, 0, s == SWEEPS - 1)
        return carry

    lax.fori_loop(0, SWEEPS, sweep, 0)
    left_basis[...] = xf[0]
    right_basis[...] = xf[1]
    o, t = rayleigh(0), transport(1)
    run("OOTTOTTTOTO", O=o, T=t)
    rest(t)
    rest(o)
    rest(rayleigh(1))


def solution(mesh):
    rows, col = mesh.shape["row"], mesh.shape["col"]

    def local_program(left_op, left_start, right_op, right_start):
        blk, s = left_op.shape[0], left_start.shape[1]
        sub = left_start.shape[0]
        vmem = pl.BlockSpec(memory_space=pltpu.VMEM)
        hbm = pl.BlockSpec(memory_space=pl.ANY)
        basis = jax.ShapeDtypeStruct((sub, s), F32)
        ray = jax.ShapeDtypeStruct((s, s), F32)
        dma = pltpu.SemaphoreType.DMA
        scratch = [
            pltpu.VMEM((2, blk, blk), BF16),
            pltpu.VMEM((2, blk, s), BF16),
            pltpu.VMEM((2, rows, sub, s), BF16),
            pltpu.VMEM((2, sub, s), F32),
            pltpu.VMEM((2, col, sub, s), F32),
            pltpu.VMEM((2, 2, sub, s), F32),
            pltpu.VMEM((2, sub, s), F32),
            pltpu.VMEM((2, sub, s), F32),
            pltpu.VMEM((2, sub, s), F32),
            pltpu.VMEM((2, 2 * s, s), F32),
            pltpu.VMEM((2, s, s), F32),
            pltpu.VMEM((2, s, s), F32),
            pltpu.VMEM((2, s // 2, s), F32),
            pltpu.VMEM((2, 2, 2 * rows, s // 2, s), F32),
            pltpu.VMEM((2, 2 * s, s), F32),
            pltpu.VMEM((2, s, 2 * s), F32),
            pltpu.VMEM((2, s, s), F32),
            pltpu.VMEM((2, 4, 8, s), F32),
            dma((2, col)),
            dma((2, 2)), dma((2, 2)), dma((2,)), dma((2,)),
            dma((2,)), dma((2,)), dma((2,)), dma((2,)),
            dma((2, 2 * rows)), dma((2, 2, 2 * rows)), dma((2,)), dma((2,)),
            dma((2, rows, CHUNKS)), dma((2, rows, CHUNKS)), dma((2, rows, CHUNKS)),
            dma((2, rows, CHUNKS)), dma((2, col, CHUNKS)),
        ]
        return pl.pallas_call(
            functools.partial(kernel, rows, col),
            out_shape=(basis, ray, basis, ray),
            in_specs=[hbm, vmem, hbm, vmem],
            out_specs=(vmem,) * 4,
            scratch_shapes=scratch,
            compiler_params=pltpu.CompilerParams(collective_id=0, has_side_effects=True, vmem_limit_bytes=66_000_000),
        )(left_op, left_start, right_op, right_start)

    op_spec = P(("batch", "row"), "col")
    vec_spec = P(("batch", "row", "col"), None)
    small_spec = P("batch", None)
    return jax.shard_map(local_program, mesh=mesh, in_specs=(op_spec, vec_spec, op_spec, vec_spec), out_specs=(vec_spec, small_spec, vec_spec, small_spec), check_vma=False)
```

```python
import functools

import jax
import jax.numpy as jnp
from jax import lax
from jax.experimental import pallas as pl
from jax.experimental.pallas import tpu as pltpu
from jax.sharding import PartitionSpec as P

SWEEPS = 4
CHUNKS = 3
PARTS = 4
MESH = pl.DeviceIdType.MESH
HIGHEST = lax.Precision.HIGHEST
OPS = (0, 1)
F32 = jnp.float32
BF16 = jnp.bfloat16


def dot(lhs, rhs, lhs_dim, rhs_dim, precision=None):
    dims = (((lhs_dim,), (rhs_dim,)), ((), ()))
    return lax.dot_general(lhs, rhs, dims, precision=precision, preferred_element_type=F32)


def split3(v):
    one = v.astype(BF16).astype(F32)
    rest = v - one
    two = rest.astype(BF16).astype(F32)
    return one, two, rest - two


def kernel(rows, col, left_op, left_start, right_op, right_start, left_basis, left_ray, right_basis, right_ray,
           a_v, xg, xz, xf, part, rsa, sb, rsb, yv, gp, g1, s1, g2, slots, gs, gw, mv, keep,
           load_sem, rsa_ss, rsa_rs, rsb_ss, rsb_rs, g1_ss, g1_rs, g2_ss, g2_rs, sl_ss, sl_rs, g4_ss, g4_rs,
           zr_ss, zl_ss, z_rs, p_ss, p_rs):
    b, z, c = lax.axis_index("batch"), lax.axis_index("row"), lax.axis_index("col")
    y, k = c // 2, c % 2
    blk = a_v.shape[1]
    sub = blk // col
    piece = sub // CHUNKS
    total = blk * rows

    def dev(zz, yy, kk):
        return (b, zz, 2 * yy + kk)

    def rcopy(src, dst, ss, rs, to):
        return pltpu.make_async_remote_copy(src_ref=src, dst_ref=dst, send_sem=ss, recv_sem=rs, device_id=to, device_id_type=MESH)

    partner, across = dev(z, y, 1 - k), dev(z, 1 - y, k)

    def load(op, j):
        src = (left_op, right_op)[op]
        rng = pl.ds(j * sub, sub)
        return pltpu.make_async_copy(src.at[rng], a_v.at[op, rng], load_sem.at[op, j])

    for op in OPS:
        for j in range(col):
            load(op, j).start()

    barrier = pltpu.get_barrier_semaphore()
    me = z * col + c
    count = rows * col
    for d in range(1, count):
        peer = lax.rem(me + d, count)
        pl.semaphore_signal(barrier, inc=1, device_id=(b, peer // col, lax.rem(peer, col)), device_id_type=MESH)
    pl.semaphore_wait(barrier, count - 1)

    def z_copy(op, slot, h, step):
        rng = pl.ds(h * piece, piece)
        to, ss = (dev(z + 1, y, k), zr_ss) if step > 0 else (dev(z - 1, y, k), zl_ss)
        return rcopy(xz.at[op, slot, rng], xz.at[op, slot, rng], ss.at[op, slot, h], z_rs.at[op, slot, h], to)

    def p_copy(op, slot, h):
        src = xz.at[op, slot, pl.ds(h * piece, piece)]
        dst = xg.at[op, pl.ds(c * sub + h * piece, piece)]
        return rcopy(src, dst, p_ss.at[op, slot, h], p_rs.at[op, c, h], dev(z, slot // 2, lax.rem(slot, 2)))

    def p_local(op, slot, h):
        src = xz.at[op, slot, pl.ds(h * piece, piece)]
        dst = xg.at[op, pl.ds(c * sub + h * piece, piece)]
        return pltpu.make_async_copy(src, dst, p_rs.at[op, c, h])

    def p_start(op, slot, h):
        @pl.when(slot == c)
        def _():
            p_local(op, slot, h).start()

        @pl.when(slot != c)
        def _():
            p_copy(op, slot, h).start()

    def spread_begin(op):
        for h in range(CHUNKS):
            @pl.when(z < rows - 1)
            def _():
                z_copy(op, z, h, 1).start()

            @pl.when(z > 0)
            def _():
                z_copy(op, z, h, -1).start()
        for h in range(CHUNKS):
            p_start(op, z, h)

    def spread_step(op, t, h):
        @pl.when(z - t >= 0)
        def _():
            slot = z - t
            z_copy(op, slot, h, 1).wait_recv()

            @pl.when(z < rows - 1)
            def _():
                z_copy(op, slot, h, 1).start()

            p_start(op, slot, h)

        @pl.when(z + t < rows)
        def _():
            slot = z + t
            z_copy(op, slot, h, -1).wait_recv()

            @pl.when(z > 0)
            def _():
                z_copy(op, slot, h, -1).start()

            p_start(op, slot, h)

    def spread_end(op):
        for src in range(col):
            for h in range(CHUNKS):
                dst = xg.at[op, pl.ds(src * sub + h * piece, piece)]
                pltpu.make_async_copy(dst, dst, p_rs.at[op, src, h]).wait()

    def spread_sent(op):
        for slot in range(rows):
            for h in range(CHUNKS):
                @pl.when((slot <= z) & (z < rows - 1))
                def _():
                    z_copy(op, slot, h, 1).wait_send()

                @pl.when((slot >= z) & (z > 0))
                def _():
                    z_copy(op, slot, h, -1).wait_send()

                @pl.when(slot != c)
                def _():
                    p_copy(op, slot, h).wait_send()

    def core_copy(op, yy):
        return rcopy(part.at[op, 2 * yy + 1 - k], rsa.at[op, yy], rsa_ss.at[op, yy], rsa_rs.at[op, yy], partner)

    def y_copy(op):
        return rcopy(sb.at[op], rsb.at[op], rsb_ss.at[op], rsb_rs.at[op], across)

    def product(op, i):
        yy, kk = (1 - y, y)[i // 2], (1 - k, k)[i % 2]
        j = 2 * yy + kk
        upper, lower = (
            dot(a_v[op, pl.ds(pl.multiple_of(j * sub + n * (sub // 2), sub // 2), sub // 2), :], xg[op], 1, 0) for n in range(2)
        )
        part[op, j, 0:sub // 2] = upper
        part[op, j, sub // 2:sub] = lower
        if i % 2 == 0:
            core_copy(op, yy).start()
        if i == 1:
            core_copy(op, yy).wait_recv()
            sb[op] = part[op, j] + rsa[op, yy]
            y_copy(op).start()

    def product_end(op):
        core_copy(op, y).wait_recv()
        own = part[op, c] + rsa[op, y]
        y_copy(op).wait_recv()
        yv[op] = own + rsb[op]
        core_copy(op, 0).wait_send()
        core_copy(op, 1).wait_send()
        y_copy(op).wait_send()

    def group_sum(op, turn, size):
        half, quarter = size // 2, size // 4

        def rng(which, length):
            return pl.ds(pl.multiple_of(which * length, length), length)

        c1 = rcopy(gp.at[op, rng(1 - k, half)], g1.at[op, pl.ds(0, half)], g1_ss.at[op], g1_rs.at[op], partner)
        c2 = rcopy(s1.at[op, rng(1 - y, quarter)], g2.at[op, pl.ds(0, quarter)], g2_ss.at[op], g2_rs.at[op], across)
        c4 = rcopy(gs.at[op, rng(k, half)], gs.at[op, rng(k, half)], g4_ss.at[op], g4_rs.at[op], partner)
        c4_in = rcopy(gs.at[op, rng(1 - k, half)], gs.at[op, rng(1 - k, half)], g4_ss.at[op], g4_rs.at[op], partner)
        chip, chips = 2 * z + y, 2 * rows

        def c3(d, mine):
            other = lax.rem(chip + d, chips)
            at = chip if mine else other
            place = slots.at[op, turn, at, pl.ds(0, quarter)]
            return rcopy(place, place, sl_ss.at[op, d], sl_rs.at[op, turn, at], dev(other // 2, lax.rem(other, 2), k))

        def over_cores():
            c1.wait_recv()
            s1[op, 0:half] = gp[op, rng(k, half), :] + g1[op, 0:half]
            c2.start()

        def over_y():
            c2.wait_recv()
            slots[op, turn, chip, 0:quarter] = s1[op, rng(y, quarter), :] + g2[op, 0:quarter]
            for d in range(1, chips):
                c3(d, True).start()

        def over_chips():
            for d in range(1, chips):
                c3(d, False).wait_recv()
            for yy in range(2):
                acc = slots[op, turn, yy, 0:quarter]
                for zz in range(1, rows):
                    acc = acc + slots[op, turn, 2 * zz + yy, 0:quarter]
                gs[op, pl.ds(pl.multiple_of(k * half + yy * quarter, quarter), quarter), :] = acc
            c4.start()

        def finish():
            c4_in.wait_recv()
            c1.wait_send()
            c2.wait_send()
            for d in range(1, chips):
                c3(d, True).wait_send()
            c4.wait_send()

        return c1.start, over_cores, over_y, over_chips, finish

    lane = lax.broadcasted_iota(jnp.int32, (8, 128), 1)
    sublane = lax.broadcasted_iota(jnp.int32, (8, 128), 0)

    def spread_row(v, j):
        return jnp.broadcast_to(v[j:j + 1], (8, 128))

    def panel(op, i, state):
        p0, p1, q0, q1 = state
        now = pl.ds(pl.multiple_of(i * 8, 8), 8)
        following = jnp.minimum(i + 1, 15) * 8
        cols = []
        for base in (i * 8, following):
            for j in range(8):
                one = jnp.sum(jnp.where(lane == base + j, p0, 0.0), axis=1, keepdims=True)
                cols.append(jnp.broadcast_to(one, (8, 128)))
        l1, l2, l3 = split3(q0)
        r1, r2, r3 = split3(jnp.concatenate([q0, q1], axis=1))
        lhs = jnp.concatenate([l1, l1, l2, l1, l2, l3], axis=0).astype(BF16)
        rhs = jnp.concatenate([r1, r2, r1, r3, r2, r1], axis=0).astype(BF16)
        gw[op] = gw[op] - dot(lhs, rhs, 0, 0)
        scale = jnp.ones((8, 128), F32)
        for j in range(8):
            root = lax.rsqrt(spread_row(cols[j], j))
            scale = jnp.where(sublane == j, root, scale)
            if j < 7:
                m = jnp.where(sublane > j, cols[j] * (root * root), 0.0)
                for q in range(j + 1, 16):
                    cols[q] = cols[q] - m * spread_row(cols[q], j)
                p0 = p0 - m * spread_row(p0, j)
                p1 = p1 - m * spread_row(p1, j)
        p0, p1 = p0 * scale, p1 * scale
        mv[op, now, :] = p1
        s0, s1_ = jnp.zeros((8, 128), F32), jnp.zeros((8, 128), F32)
        for j in range(8):
            w = cols[8 + j] * scale
            s0 = jnp.where(sublane == j, jnp.sum(w * p0, axis=0, keepdims=True), s0)
            s1_ = jnp.where(sublane == j, jnp.sum(w * p1, axis=0, keepdims=True), s1_)
        rng = pl.ds(pl.multiple_of(following, 8), 8)
        return gw[op, rng, 0:128] - s0, gw[op, rng, 128:256] - s1_, p0, p1

    def factor(op):
        zero = jnp.zeros((8, 128), F32)
        state = (gw[op, 0:8, 0:128], gw[op, 0:8, 128:256], zero, zero)
        for part_no in range(PARTS):
            if part_no:
                yield
                state = tuple(keep[op, i] for i in range(4))
            n = 16 // PARTS
            state = lax.fori_loop(n * part_no, n * part_no + n, lambda i, st: panel(op, i, st), state)
            if part_no < PARTS - 1:
                for i in range(4):
                    keep[op, i] = state[i]

    def eye():
        return (lax.broadcasted_iota(jnp.int32, (128, 128), 0) == lax.broadcasted_iota(jnp.int32, (128, 128), 1)).astype(F32)

    def transport(op, first=False):
        for n in range((rows - 1) * CHUNKS):
            spread_step(op, n // CHUNKS + 1, n % CHUNKS)
            yield
        if first:
            for j in range(col):
                load(op, j).wait()
        spread_end(op)
        for i in range(4):
            product(op, i)
            yield
        spread_sent(op)

    def ortho(op, last):
        product_end(op)
        y_cur = yv[op]
        y_half = y_cur.astype(BF16)
        gp[op, 0:128] = dot(y_half, y_half, 0, 0)
        gp[op, 128:256] = dot(y_cur, y_cur, 0, 0, HIGHEST)
        steps = group_sum(op, 0, 256)
        steps[0]()
        for step in steps[1:-1]:
            yield
            step()
        yield
        steps[-1]()
        gw[op, :, 0:128] = gs[op, 0:128] / total
        gw[op, :, 128:256] = eye()
        yield from factor(op)
        yield
        steps = group_sum(op, 1, 128)

        @pl.when(last)
        def _():
            y_one = dot(yv[op], mv[op], 1, 1, HIGHEST)
            yv[op] = y_one
            gp[op, 0:128] = dot(y_one, y_one, 0, 0, HIGHEST)
            steps[0]()

        @pl.when(jnp.logical_not(last))
        def _():
            inv = mv[op]
            gw[op, :, 0:128] = dot(dot(inv, gs[op, 128:256] / total, 1, 0, HIGHEST), inv, 1, 1, HIGHEST)
            gw[op, :, 128:256] = inv

        for step in steps[1:-1]:
            yield
            pl.when(last)(step)
        yield

        @pl.when(last)
        def _():
            steps[-1]()
            gw[op, :, 0:128] = gs[op, 0:128] / total
            gw[op, :, 128:256] = eye()

        yield from factor(op)
        halves = [dot(yv[op, n * (sub // 2):(n + 1) * (sub // 2)], mv[op], 1, 1, HIGHEST) for n in range(2)]
        for n, x in enumerate(halves):
            rng = slice(n * (sub // 2), (n + 1) * (sub // 2))
            xf[op, rng] = x
            xz[op, z, rng] = x.astype(BF16)
        spread_begin(op)

    def rayleigh(op):
        product_end(op)
        gp[op, 0:128] = dot(xf[op], yv[op], 0, 0, HIGHEST)
        steps = group_sum(op, 0, 128)
        steps[0]()
        for step in steps[1:]:
            yield
            step()
        (left_ray, right_ray)[op][...] = gs[op, 0:128] / total

    def run(order, **streams):
        for name in order:
            next(streams[name], None)

    def rest(stream):
        for _ in stream:
            pass

    def half_sweep(o_op, t_op, last):
        o, t = ortho(o_op, last), transport(t_op)
        run("OOTTTOTTTTTOTOOTTOOOOTOTOOO", O=o, T=t)
        rest(t)
        rest(o)

    xz[0, z] = left_start[...].astype(BF16)
    spread_begin(0)
    xz[1, z] = right_start[...].astype(BF16)
    t = transport(0, True)
    run("T" * ((rows - 1) * CHUNKS), T=t)
    spread_begin(1)
    rest(t)
    for j in range(col):
        load(1, j).wait()

    def sweep(s, carry):
        half_sweep(0, 1, s == SWEEPS - 1)
        half_sweep(1, 0, s == SWEEPS - 1)
        return carry

    lax.fori_loop(0, SWEEPS, sweep, 0)
    left_basis[...] = xf[0]
    right_basis[...] = xf[1]
    o, t = rayleigh(0), transport(1)
    run("OOTTTOTTTTTOTO", O=o, T=t)
    rest(t)
    rest(o)
    rest(rayleigh(1))


def solution(mesh):
    rows, col = mesh.shape["row"], mesh.shape["col"]

    def local_program(left_op, left_start, right_op, right_start):
        blk, s = left_op.shape[0], left_start.shape[1]
        sub = left_start.shape[0]
        vmem = pl.BlockSpec(memory_space=pltpu.VMEM)
        hbm = pl.BlockSpec(memory_space=pl.ANY)
        basis = jax.ShapeDtypeStruct((sub, s), F32)
        ray = jax.ShapeDtypeStruct((s, s), F32)
        dma = pltpu.SemaphoreType.DMA
        scratch = [
            pltpu.VMEM((2, blk, blk), BF16),
            pltpu.VMEM((2, blk, s), BF16),
            pltpu.VMEM((2, rows, sub, s), BF16),
            pltpu.VMEM((2, sub, s), F32),
            pltpu.VMEM((2, col, sub, s), F32),
            pltpu.VMEM((2, 2, sub, s), F32),
            pltpu.VMEM((2, sub, s), F32),
            pltpu.VMEM((2, sub, s), F32),
            pltpu.VMEM((2, sub, s), F32),
            pltpu.VMEM((2, 2 * s, s), F32),
            pltpu.VMEM((2, s, s), F32),
            pltpu.VMEM((2, s, s), F32),
            pltpu.VMEM((2, s // 2, s), F32),
            pltpu.VMEM((2, 2, 2 * rows, s // 2, s), F32),
            pltpu.VMEM((2, 2 * s, s), F32),
            pltpu.VMEM((2, s, 2 * s), F32),
            pltpu.VMEM((2, s, s), F32),
            pltpu.VMEM((2, 4, 8, s), F32),
            dma((2, col)),
            dma((2, 2)), dma((2, 2)), dma((2,)), dma((2,)),
            dma((2,)), dma((2,)), dma((2,)), dma((2,)),
            dma((2, 2 * rows)), dma((2, 2, 2 * rows)), dma((2,)), dma((2,)),
            dma((2, rows, CHUNKS)), dma((2, rows, CHUNKS)), dma((2, rows, CHUNKS)),
            dma((2, rows, CHUNKS)), dma((2, col, CHUNKS)),
        ]
        return pl.pallas_call(
            functools.partial(kernel, rows, col),
            out_shape=(basis, ray, basis, ray),
            in_specs=[hbm, vmem, hbm, vmem],
            out_specs=(vmem,) * 4,
            scratch_shapes=scratch,
            compiler_params=pltpu.CompilerParams(collective_id=0, has_side_effects=True, vmem_limit_bytes=66_000_000),
        )(left_op, left_start, right_op, right_start)

    op_spec = P(("batch", "row"), "col")
    vec_spec = P(("batch", "row", "col"), None)
    small_spec = P("batch", None)
    return jax.shard_map(local_program, mesh=mesh, in_specs=(op_spec, vec_spec, op_spec, vec_spec), out_specs=(vec_spec, small_spec, vec_spec, small_spec), check_vma=False)
```
